32 devices in a mesh: lat: 4 (over z), lon: 8 (over y, x, core).
Axes of the slice: x: 2, y: 2, z: 4, core: 2. Of those that a mesh axis runs over, the one named last changes fastest.
Arguments:
- poleward_flow: float32 [10, 4, 256, 1024], P(None, None, 'lat', 'lon'), may hold values from -16 to 16
- potential_warmth: float32 [10, 4, 256, 1024], P(None, None, 'lat', 'lon'), may hold values from -16 to 16
- water_profile_flag: int32 [256, 1024], P('lat', 'lon'), may hold values from 0 to 1
- floor_count: int32 [256, 1024], P('lat', 'lon'), may hold values from 0 to 4, as said below
- catchment_label_for_site: int32 [256, 1024], P('lat', 'lon'), may hold values from 0 to 9
Outputs:
- eddy_temp: float32 [4, 256, 1024], P(None, 'lat', 'lon')
- transport: float32 [4, 10, 4, 256], P(None, None, None, ('lat', 'lon'))
The draws below stay inside these ranges and needn't reach their ends.
Inputs may be any that keep to these rules, and one draw needn't show every extreme that they name: `floor_count`: land rows of zeros occur at some latitudes; elsewhere columns have 1 to 4 wet levels.
All inputs are finite; a program needn't handle non-finite values.
Results may differ from the reference program's by a relative error of at most 0.0003.
Values sent between devices are 32-bit elements; how exact they have to be, the bound alone decides.
A program may use at most 64 MiB of HBM per device.

```python
import math
import jax
import jax.numpy as jnp
from jax import lax

SNAPSHOT_TIMES = 10
LAYERS = 4
BASINS = 10
MERIDIAN_POINTS = 256
LONGITUDE_SLOTS = 1024


def ocean_fields(key):
    generator_keys = jax.random.split(jax.random.fold_in(key, 11), 10)
    along_latitude_flow = jax.random.normal(generator_keys[0], (1, LAYERS, MERIDIAN_POINTS, 1), jnp.float32)
    along_latitude_warmth = jax.random.normal(generator_keys[1], (1, LAYERS, MERIDIAN_POINTS, 1), jnp.float32)
    residual_transport_term = jax.random.normal(generator_keys[2], (SNAPSHOT_TIMES, LAYERS, MERIDIAN_POINTS, 1), jnp.float32)
    thermal_deviate = 0.6 * residual_transport_term + 0.8 * jax.random.normal(generator_keys[3], (SNAPSHOT_TIMES, LAYERS, MERIDIAN_POINTS, 1), jnp.float32)
    steady_share = jax.random.normal(generator_keys[4], (1, LAYERS, MERIDIAN_POINTS, LONGITUDE_SLOTS), jnp.float32)
    steady_warmth = jax.random.normal(generator_keys[5], (1, LAYERS, MERIDIAN_POINTS, LONGITUDE_SLOTS), jnp.float32)
    speed_residual = jax.random.normal(generator_keys[6], (SNAPSHOT_TIMES, LAYERS, MERIDIAN_POINTS, LONGITUDE_SLOTS), jnp.float32)
    thermal_residual = jax.random.normal(generator_keys[7], (SNAPSHOT_TIMES, LAYERS, MERIDIAN_POINTS, LONGITUDE_SLOTS), jnp.float32)
    steady_factor = jax.random.uniform(generator_keys[8], (1, LAYERS, MERIDIAN_POINTS, 1), jnp.float32, -1.0, 1.0)
    fluctuating_factor = jax.random.uniform(generator_keys[9], (1, LAYERS, MERIDIAN_POINTS, 1), jnp.float32, 0.2, 1.0)
    poleward_flow = 0.5 * along_latitude_flow + 0.3 * residual_transport_term + 0.7 * steady_share + speed_residual
    potential_warmth = along_latitude_warmth + 0.3 * thermal_deviate + steady_factor * steady_share + 0.5 * steady_warmth + fluctuating_factor * speed_residual + 0.6 * thermal_residual
    return (jnp.clip(poleward_flow, -16.0, 16.0), jnp.clip(potential_warmth, -16.0, 16.0))


def draw_poleward_flow(key, part):
    return ocean_fields(key)[0]


def draw_potential_warmth(key, part):
    return ocean_fields(key)[1]


def draw_water_profile_flag(key, part):
    columns = jnp.arange(LONGITUDE_SLOTS, dtype=jnp.int32)
    threshold = 25 + 65 * columns // LONGITUDE_SLOTS
    dice = jax.random.randint(jax.random.fold_in(key, 21), (MERIDIAN_POINTS, LONGITUDE_SLOTS), 0, 100)
    return (dice < threshold[None, :]).astype(jnp.int32)


def draw_floor_count(key, part):
    wet_levels = jax.random.randint(jax.random.fold_in(key, 31), (MERIDIAN_POINTS, LONGITUDE_SLOTS), 1, LAYERS + 1)
    land_rows = jax.random.randint(jax.random.fold_in(key, 32), (MERIDIAN_POINTS, 1), 0, 16) == 0
    return jnp.where(land_rows, 0, wet_levels).astype(jnp.int32)


def touch_ends(entries, own_key, low, top_value):
    dims = entries.shape
    index_at = [jax.random.randint(jax.random.fold_in(own_key, axis), (), 0, dims[axis]) for axis in range(len(dims))]
    entries = entries.at[tuple(index_at)].set(low)
    longest = dims.index(max(dims))
    index_at[longest] = (index_at[longest] + 1) % dims[longest]
    return entries.at[tuple(index_at)].set(top_value)


def setup_inputs(seed: int = 0) -> dict:
    key_of = jax.random.split(jax.random.key(seed), 6)
    return {
        "poleward_flow": draw_poleward_flow(jax.random.fold_in(key_of[5], 71), 0),
        "potential_warmth": draw_potential_warmth(jax.random.fold_in(key_of[5], 71), 0),
        "water_profile_flag": draw_water_profile_flag(jax.random.fold_in(key_of[5], 71), 0),
        "floor_count": draw_floor_count(jax.random.fold_in(key_of[5], 71), 0),
        "catchment_label_for_site": touch_ends(jax.random.randint(key_of[4], (MERIDIAN_POINTS, LONGITUDE_SLOTS), 0, BASINS), jax.random.fold_in(key_of[4], 1), 0, BASINS - 1).astype(jnp.int32),
    }


highest_accuracy = lax.Precision.HIGHEST

def layer_summands(layer_position, meridional_speed_layer, thermal_layer_slice, bottom_layer_limit, catchment_label_for_site):
    topmost_warmth = jnp.concatenate([thermal_layer_slice[:, 1:, :], jnp.zeros_like(thermal_layer_slice[:, :1, :])], axis=1)
    warmth_entry = 0.5 * (thermal_layer_slice + topmost_warmth)
    upper_depth = jnp.concatenate([bottom_layer_limit[1:], jnp.zeros_like(bottom_layer_limit[:1])], axis=0)
    level_value = layer_position.astype(jnp.float32)
    wet_cells = ((level_value < bottom_layer_limit) & (level_value < upper_depth)).astype(jnp.float32)
    basin_ids = jnp.arange(BASINS, dtype=jnp.int32)
    one_hot = (catchment_label_for_site[None] == basin_ids[:, None, None]).astype(jnp.float32)
    scaling_factors = one_hot * wet_cells[None]
    watered_total = lax.optimization_barrier(jnp.sum(scaling_factors, axis=2))
    along_latitude_flow = jnp.einsum('qfd,zfd->zqf', scaling_factors, meridional_speed_layer, precision=highest_accuracy)
    along_latitude_warmth = jnp.einsum('qfd,zfd->zqf', scaling_factors, warmth_entry, precision=highest_accuracy)
    means_v = along_latitude_flow / jnp.maximum(watered_total, 1.0)
    averages_heat = along_latitude_warmth / jnp.maximum(watered_total, 1.0)
    bar_v = lax.optimization_barrier(jnp.mean(means_v, axis=0))
    bar_t = lax.optimization_barrier(jnp.mean(averages_heat, axis=0))
    mean_velocity = lax.optimization_barrier(jnp.mean(meridional_speed_layer, axis=0))
    average_warmth = lax.optimization_barrier(jnp.mean(warmth_entry, axis=0))
    bar_v_cells = jnp.einsum('bji,bj->ji', one_hot, bar_v, precision=highest_accuracy)
    averaged_heat_grid = jnp.einsum('bji,bj->ji', one_hot, bar_t, precision=highest_accuracy)
    means_v_cells = jnp.einsum('bji,tbj->tji', one_hot, means_v, precision=highest_accuracy)
    averages_heat_grid = jnp.einsum('bji,tbj->tji', one_hot, averages_heat, precision=highest_accuracy)
    velocity_star = mean_velocity - bar_v_cells
    temp_star = average_warmth - averaged_heat_grid
    velocity_eddy = meridional_speed_layer - mean_velocity - (means_v_cells - bar_v_cells)
    warmth_fluctuation = warmth_entry - average_warmth - (averages_heat_grid - averaged_heat_grid)
    scaling = 1.0 / math.sqrt(LONGITUDE_SLOTS)
    mean_flow = scaling * watered_total * bar_v * bar_t
    steady_share = scaling * jnp.einsum('bji,ji->bj', scaling_factors, velocity_star * temp_star, precision=highest_accuracy)
    zonal_swing = scaling * watered_total * lax.optimization_barrier(jnp.mean((means_v - bar_v) * (averages_heat - bar_t), axis=0))
    transient = scaling * jnp.einsum('bji,ji->bj', scaling_factors, lax.optimization_barrier(jnp.mean(velocity_eddy * warmth_fluctuation, axis=0)), precision=highest_accuracy)
    return (wet_cells * temp_star, jnp.stack([mean_flow, steady_share, zonal_swing, transient]))

def reference(poleward_flow, potential_warmth, water_profile_flag, floor_count, catchment_label_for_site):
    bottom_layer_limit = (water_profile_flag * floor_count).astype(jnp.float32)

    def per_level(layer_position):
        meridional_speed_layer = lax.dynamic_index_in_dim(poleward_flow, layer_position, 1, keepdims=False)
        thermal_layer_slice = lax.dynamic_index_in_dim(potential_warmth, layer_position, 1, keepdims=False)
        return layer_summands(layer_position, meridional_speed_layer, thermal_layer_slice, bottom_layer_limit, catchment_label_for_site)
    eddy_temp, stacked = lax.map(per_level, jnp.arange(LAYERS, dtype=jnp.int32))
    return (eddy_temp, jnp.transpose(stacked, (1, 2, 0, 3)))
```

```python
import functools
import math

import jax
import jax.numpy as jnp
from jax import lax
from jax.experimental import pallas as pl
from jax.experimental.pallas import tpu as pltpu
from jax.sharding import PartitionSpec as P

BASINS = 10
MESH = pl.DeviceIdType.MESH
SUB = 8
LANES = 128
GROUPS = 2


def kernel(
    lat_devices, lon_devices, snapshots, levels, share_rows,
    flow_hbm, warmth_hbm, flag_hbm, floor_hbm, label_hbm,
    eddy_ref, transport_ref,
    columns, depth, flow, warmth, average, dots,
    halo_out, halo_in, stats, pair_stats, chip_stats, received, chip_sums, peer_sums, all_sums,
    edge_sums, peer_edge, edge_stats, peer_edge_stats, edge_total, edge_stats_total,
    load_first, load_columns, load_rest, halo_send, halo_recv,
    pair_send, pair_recv, stat_send, stat_recv, sum_send, sum_recv, share_send, share_recv,
    edge_send, edge_recv, edge_stat_send, edge_stat_recv,
):
    rows = flow.shape[1]
    blocks = rows // SUB
    last = blocks - 1
    half_blocks = blocks // GROUPS
    label_ref = columns.at[2]
    owners = SUB // share_rows
    planes = snapshots * levels
    parities, slots, packed = stats.shape[:3]
    group_slots = slots // GROUPS
    fields = dots.shape[1] // SUB
    used = BASINS * SUB
    chips = lon_devices // 2
    lat = lax.axis_index("lat")
    me = lax.axis_index("lon")
    core = lax.rem(me, 2)
    chip = me // 2
    mine = core if parities == 2 else 0
    theirs = 1 - core if parities == 2 else 0
    partner = (lat, me + 1 - 2 * core)
    own_slot = me // (owners * parities)
    scaling = 1.0 / math.sqrt(LANES * lon_devices)
    has_next = lat < lat_devices - 1

    def window(b):
        return pl.ds(b * SUB, SUB)

    def flow_copy(b):
        at = window(b)
        return pltpu.make_async_copy(flow_hbm.at[:, at, :], flow.at[:, at, :], load_rest.at[b // half_blocks])

    def warmth_copy(b):
        at = window(b)
        sem = load_first if b == 0 else load_rest.at[(b - 1) // half_blocks]
        return pltpu.make_async_copy(warmth_hbm.at[:, at, :], warmth.at[:, at, :], sem)

    def await_bytes(ref, sem):
        pltpu.make_async_copy(ref, ref, sem).wait()

    warmth_copy(0).start()
    for n, column in enumerate((flag_hbm, floor_hbm, label_hbm)):
        pltpu.make_async_copy(column, columns.at[n], load_columns).start()
    for g in range(GROUPS):
        for b in range(g * half_blocks, (g + 1) * half_blocks):
            flow_copy(b).start()
            if b < last:
                warmth_copy(b + 1).start()

    barrier = pltpu.get_barrier_semaphore()

    def greet(d, carry):
        pl.semaphore_signal(
            barrier, inc=1, device_id=(lat, lax.rem(me + d, lon_devices)), device_id_type=MESH
        )
        return carry

    @pl.when(has_next)
    def _():
        pl.semaphore_signal(barrier, inc=1, device_id=(lat + 1, me), device_id_type=MESH)

    lax.fori_loop(1, lon_devices, greet, 0)

    halo_copy = pltpu.make_async_remote_copy(
        src_ref=halo_out, dst_ref=halo_in, send_sem=halo_send, recv_sem=halo_recv,
        device_id=(jnp.maximum(lat - 1, 0), me), device_id_type=MESH,
    )

    def group(g):
        return pl.ds(g * group_slots, group_slots)

    def pair_copy(g):
        return pltpu.make_async_remote_copy(
            src_ref=stats.at[theirs, group(g)], dst_ref=pair_stats.at[group(g)],
            send_sem=pair_send, recv_sem=pair_recv.at[g],
            device_id=partner, device_id_type=MESH,
        )

    def sum_copy(g, to, source):
        return pltpu.make_async_remote_copy(
            src_ref=chip_sums.at[group(g)], dst_ref=peer_sums.at[source, group(g)],
            send_sem=sum_send, recv_sem=sum_recv,
            device_id=(lat, 2 * to + core), device_id_type=MESH,
        )

    def stat_slot(to):
        return (2 * to + core) // (owners * parities)

    def stat_copy(to, source):
        return pltpu.make_async_remote_copy(
            src_ref=chip_stats.at[stat_slot(to)], dst_ref=received.at[source],
            send_sem=stat_send, recv_sem=stat_recv,
            device_id=(lat, 2 * to + core), device_id_type=MESH,
        )

    share_copy = pltpu.make_async_remote_copy(
        src_ref=all_sums.at[mine], dst_ref=all_sums.at[mine],
        send_sem=share_send, recv_sem=share_recv, device_id=partner, device_id_type=MESH,
    )

    def edge_copy(to, source):
        return pltpu.make_async_remote_copy(
            src_ref=edge_sums, dst_ref=peer_edge.at[source],
            send_sem=edge_send, recv_sem=edge_recv,
            device_id=(lat, to), device_id_type=MESH,
        )

    def edge_stat_copy(source):
        return pltpu.make_async_remote_copy(
            src_ref=edge_stats, dst_ref=peer_edge_stats.at[source],
            send_sem=edge_stat_send, recv_sem=edge_stat_recv,
            device_id=(lat, lon_devices - 1), device_id_type=MESH,
        )

    def each_chip(action):
        def step(d, carry):
            action(lax.rem(chip + d, chips))
            return carry

        lax.fori_loop(1, chips, step, 0)

    def each_peer(action):
        def step(d, carry):
            action(lax.rem(me + d, lon_devices))
            return carry

        lax.fori_loop(1, lon_devices, step, 0)

    sub = lax.broadcasted_iota(jnp.int32, (SUB, LANES), 0)
    level = lax.broadcasted_iota(jnp.int32, (levels, SUB, LANES), 0).astype(jnp.float32)

    def next_row(here, after):
        first = lax.broadcasted_iota(jnp.int32, here.shape, here.ndim - 2) == 0
        return pltpu.roll(jnp.where(first, after, here), SUB - 1, here.ndim - 2)

    def both_halves(x):
        return x + pltpu.roll(x, levels, 0)

    def wet_cells(b):
        here = depth[window(b), :]
        limit = jnp.minimum(here, next_row(here, depth[window(b + 1), :]))
        return (level < limit[None]).astype(jnp.float32)

    def split_dot(values, member, out_rows):
        high = values.astype(jnp.bfloat16)
        low = (values - high.astype(jnp.float32)).astype(jnp.bfloat16)
        return lax.dot_general(
            jnp.concatenate([high, low], axis=1), jnp.concatenate([member, member], axis=1),
            (((1,), (1,)), ((), ())), preferred_element_type=jnp.float32,
        )

    def block_stats(b):
        at = window(b)
        wet = wet_cells(b)
        velocity = flow[:, at, :].reshape(snapshots, levels, SUB, LANES)
        here = warmth[:, at, :]
        point = (0.5 * (here + next_row(here, warmth[:, window(b + 1), :]))).reshape(
            snapshots, levels, SUB, LANES
        )
        mean_velocity = jnp.sum(velocity, axis=0) * (1.0 / snapshots)
        mean_warmth = jnp.sum(point, axis=0) * (1.0 / snapshots)
        cross = jnp.sum((velocity - mean_velocity) * (point - mean_warmth), axis=0) * (1.0 / snapshots)
        average[:, at, :] = mean_warmth
        values = jnp.concatenate(
            [
                (point * wet[None]).reshape(planes, SUB, LANES),
                wet,
                wet,
                (velocity * wet[None]).reshape(planes, SUB, LANES),
                mean_velocity * mean_warmth * wet,
                cross * wet,
            ],
            axis=0,
        ).reshape(-1, LANES)
        labels = label_ref[at, :]
        member = jnp.concatenate(
            [(labels == n).astype(jnp.float32) for n in range(LANES // SUB)], axis=0
        ).astype(jnp.bfloat16)
        dots[b] = split_dot(values, member, fields * SUB)
        row_of = lax.rem(lax.broadcasted_iota(jnp.int32, (fields, LANES), 1), SUB)
        zonal = dots[b, pl.ds(0, fields, stride=SUB), :]
        for j in range(1, SUB):
            zonal = jnp.where(row_of == j, dots[b, pl.ds(j, fields, stride=SUB), :], zonal)
        half = packed // 2
        rest = zonal[packed:]
        spare = lax.broadcasted_iota(jnp.int32, (half, LANES), 1) >= used
        stats[b % parities, b // parities] = jnp.concatenate(
            [
                jnp.where(spare, pltpu.roll(rest, used, 1), zonal[:half]),
                jnp.where(spare, pltpu.roll(rest, 2 * used - LANES, 1), zonal[half:packed]),
            ],
            axis=0,
        )

    def sums_of(zonal):
        warmth_sum = both_halves(jnp.sum(zonal[:planes].reshape(planes // SUB, SUB, LANES), axis=0))
        return jnp.where(sub < levels, warmth_sum, zonal[planes : planes + SUB])

    def pair_sums(g):
        pair_copy(g).wait_recv()
        for s in range(g * group_slots, (g + 1) * group_slots):
            total = stats[mine, s] + pair_stats[s]
            chip_stats[s] = total
            chip_sums[s] = sums_of(total)

    def send_group(g):
        each_chip(lambda to: sum_copy(g, to, chip).start())

        def send_stats(to):
            @pl.when(stat_slot(to) // group_slots == g)
            def _():
                stat_copy(to, chip).start()

        each_chip(send_stats)

    warmth_copy(0).wait()
    await_bytes(columns, load_columns)
    depth[pl.ds(0, rows), :] = (columns[0] * columns[1]).astype(jnp.float32)
    depth[pl.ds(rows, SUB), :] = jnp.zeros((SUB, LANES), jnp.float32)
    warmth[:, rows, :] = jnp.zeros((planes, LANES), jnp.float32)
    halo_out[pl.ds(0, planes), :] = warmth[:, 0, :]
    halo_out[pl.ds(planes, SUB), :] = depth[pl.ds(0, SUB), :]

    pl.semaphore_wait(barrier, lon_devices - 1 + (lat > 0).astype(jnp.int32))

    @pl.when(lat > 0)
    def _():
        halo_copy.start()

    def load_group(g):
        count = half_blocks * SUB
        await_bytes(flow.at[:, pl.ds(g * count, count), :], load_rest.at[g])
        count = (half_blocks if g < GROUPS - 1 else half_blocks - 1) * SUB
        await_bytes(warmth.at[:, pl.ds(0, count), :], load_rest.at[g])

    load_group(0)
    for b in range(half_blocks):
        block_stats(b)
    pair_copy(0).start()
    load_group(1)
    for b in range(half_blocks, blocks):
        block_stats(b)
    pair_copy(1).start()
    pair_sums(0)
    send_group(0)
    pair_sums(1)
    send_group(1)

    lanes = lax.broadcasted_iota(jnp.int32, (SUB, LANES), 1)
    edge_total[...] = jnp.zeros((SUB, LANES), jnp.float32)
    edge_stats_total[...] = jnp.zeros((2 * SUB, LANES), jnp.float32)

    @pl.when(has_next)
    def _():
        at = rows - 1
        members = lax.broadcasted_iota(jnp.int32, (LANES, LANES), 0)
        chosen = jnp.logical_and(
            lax.rem(members, SUB) == SUB - 1, label_ref[pl.ds(at, 1), :] == members // SUB
        )
        member = chosen.astype(jnp.float32).astype(jnp.bfloat16)
        velocity = flow[:, at, :].reshape(planes // SUB, SUB, LANES)
        mean_velocity = both_halves(jnp.sum(velocity, axis=0)) * (1.0 / snapshots)
        here = warmth[:, at, :]
        halo_copy.wait_recv()
        limit = jnp.minimum(depth[pl.ds(at, 1), :], halo_in[pl.ds(planes, 1), :])
        wet = (lax.rem(sub, levels).astype(jnp.float32) < limit).astype(jnp.float32)
        point = (0.5 * (here + halo_in[pl.ds(0, planes), :])).reshape(planes // SUB, SUB, LANES)
        mean_warmth = both_halves(jnp.sum(point, axis=0)) * (1.0 / snapshots)
        cross = both_halves(
            jnp.sum((velocity - mean_velocity) * (point - mean_warmth), axis=0)
        ) * (1.0 / snapshots)
        average[:, at, :] = mean_warmth[:levels]
        depth[pl.ds(rows, SUB), :] = halo_in[pl.ds(planes, SUB), :]
        values = jnp.concatenate(
            [
                (point * wet).reshape(planes, LANES),
                wet,
                (velocity * wet).reshape(planes, LANES),
                jnp.where(sub < levels, mean_velocity * mean_warmth, cross) * wet,
            ],
            axis=0,
        )
        zonal = split_dot(values, member, fields)
        edge_sums[...] = sums_of(zonal)
        each_peer(lambda to: edge_copy(to, me).start())
        parts = [zonal[SUB * n : SUB * (n + 1)] for n in range(fields // SUB)]
        first = parts[0]
        for n in range(1, SUB):
            first = first + pltpu.roll(parts[n], LANES - n, 1)
        second = parts[SUB]
        for n in range(SUB + 1, fields // SUB):
            second = second + pltpu.roll(parts[n], LANES - (n - SUB), 1)
        edge_stats[...] = jnp.concatenate([first, second], axis=0)

        @pl.when(me < lon_devices - 1)
        def _():
            edge_stat_copy(me).start()

    def block_eddy(b, block_sums):
        at = pl.ds(b * SUB, SUB)
        wet = wet_cells(b)
        index = label_ref[at, :] * SUB + sub
        bar = block_sums / jnp.maximum(pltpu.roll(block_sums, levels, 0), 1.0) * (1.0 / snapshots)
        for k in range(levels):
            cells = jnp.take_along_axis(
                jnp.broadcast_to(bar[k : k + 1], (SUB, LANES)), index, axis=1
            )
            eddy_ref[k, at, :] = wet[k] * (average[k, at, :] - cells)

    def add_sums(d, total):
        source = lax.rem(chip + chips - d, chips)
        return total + peer_sums[pl.ds(source, 1)][0]

    await_bytes(peer_sums.at[pl.ds(0, chips - 1)], sum_recv)
    all_sums[mine] = lax.fori_loop(1, chips, add_sums, chip_sums[...], unroll=chips <= SUB)
    if parities == 2:
        share_copy.start()

    def add_received(d, total):
        source = lax.rem(chip + chips - d, chips)
        return total + received[pl.ds(source, 1)][0]

    await_bytes(received.at[pl.ds(0, chips - 1)], stat_recv)
    total = lax.fori_loop(
        1, chips, add_received, chip_stats[pl.ds(own_slot, 1)][0], unroll=chips <= SUB
    )
    if parities == 2:
        share_copy.wait_recv()
    for b in range(last):
        block_eddy(b, all_sums[b % parities, b // parities])

    @pl.when(has_next)
    def _():
        def add_edge(d, total):
            source = lax.rem(me + lon_devices - d, lon_devices)
            return total + peer_edge[pl.ds(source, 1)][0]

        await_bytes(peer_edge.at[pl.ds(0, lon_devices - 1)], edge_recv)
        edge_total[...] = lax.fori_loop(
            1, lon_devices, add_edge, edge_sums[...], unroll=lon_devices <= SUB
        )

        @pl.when(me == lon_devices - 1)
        def _():
            def add_edge_stats(d, total):
                source = lax.rem(me + lon_devices - d, lon_devices)
                return total + peer_edge_stats[pl.ds(source, 1)][0]

            await_bytes(peer_edge_stats.at[pl.ds(0, lon_devices - 1)], edge_stat_recv)
            edge_stats_total[...] = lax.fori_loop(
                1, lon_devices, add_edge_stats, edge_stats[...], unroll=lon_devices <= SUB
            )

    block_eddy(last, all_sums[last % parities, last // parities] + edge_total[...])
    half = packed // 2
    lane = lax.broadcasted_iota(jnp.int32, (half, LANES), 1)
    total = jnp.concatenate(
        [
            total,
            jnp.where(
                lane < LANES - used,
                pltpu.roll(total[:half], LANES - used, 1),
                pltpu.roll(total[half:], 2 * LANES - 2 * used, 1),
            ),
        ],
        axis=0,
    )
    extra = edge_stats_total[...]
    edge_lane = lax.rem(lanes, SUB) == SUB - 1
    pieces = []
    for n in range(fields // SUB):
        part = extra[:SUB] if n < SUB else extra[SUB:]
        if n % SUB:
            part = pltpu.roll(part, n % SUB, 1)
        pieces.append(total[SUB * n : SUB * (n + 1)] + jnp.where(edge_lane, part, 0.0))
    shape = (planes // SUB, SUB, LANES)
    per = planes // SUB
    count = pieces[per]
    divisor = jnp.maximum(count, 1.0)
    means_t = jnp.stack(pieces[:per]) / divisor
    means_v = jnp.stack(pieces[per + 1 : 2 * per + 1]) / divisor
    bar_v = both_halves(jnp.sum(means_v, axis=0)) * (1.0 / snapshots)
    bar_t = both_halves(jnp.sum(means_t, axis=0)) * (1.0 / snapshots)
    swing = both_halves(jnp.sum((means_v - bar_v) * (means_t - bar_t), axis=0)) * (1.0 / snapshots)
    upper = jnp.where(sub < levels, scaling * count * bar_v * bar_t, scaling * count * swing)
    lower = scaling * pieces[2 * per + 1] - upper
    if owners > 1:
        shift = LANES - lax.rem(me, owners) * share_rows
        upper = pltpu.roll(upper, shift, 1)
        lower = pltpu.roll(lower, shift, 1)
    spread = lax.rem(lanes * SUB + sub, LANES)
    for c, part in enumerate((upper, lower, upper, lower)):
        for k in range(levels):
            row = c // 2 * levels + k
            table = jnp.take_along_axis(
                jnp.broadcast_to(part[row : row + 1], (SUB, LANES)), spread, axis=1
            )
            transport_ref[c, k] = table[:share_rows, :BASINS]

    @pl.when(lat > 0)
    def _():
        halo_copy.wait_send()

    await_bytes(pair_stats, pair_send)
    await_bytes(peer_sums.at[pl.ds(0, chips - 1)], sum_send)
    await_bytes(received.at[pl.ds(0, chips - 1)], stat_send)
    if parities == 2:
        share_copy.wait_send()

    @pl.when(has_next)
    def _():
        await_bytes(peer_edge.at[pl.ds(0, lon_devices - 1)], edge_send)

        @pl.when(me < lon_devices - 1)
        def _():
            edge_stat_copy(me).wait_send()


def store(eddy_ref, transport_ref, eddy_hbm, transport_hbm, sems):
    copies = (
        pltpu.make_async_copy(eddy_ref, eddy_hbm, sems.at[0]),
        pltpu.make_async_copy(transport_ref, transport_hbm, sems.at[1]),
    )
    for copy in copies:
        copy.start()
    for copy in copies:
        copy.wait()


def shards(
    lat_devices, lon_devices,
    poleward_flow, potential_warmth, water_profile_flag, floor_count, catchment_label_for_site,
):
    snapshots, levels, rows, columns = poleward_flow.shape
    share_rows = rows // lon_devices
    blocks = rows // SUB
    planes = snapshots * levels
    fields = 2 * planes + 4 * levels
    packed = fields * 2 // 3
    chips = lon_devices // 2
    parities = 2 if share_rows == SUB else 1
    slots = blocks // parities
    f32, i32, vmem, dma = jnp.float32, jnp.int32, pltpu.VMEM, pltpu.SemaphoreType.DMA
    eddy_shape = (levels, rows, columns)
    transport_shape = (4, levels, share_rows, BASINS)
    eddy_temp, transport = pl.pallas_call(
        functools.partial(kernel, lat_devices, lon_devices, snapshots, levels, share_rows),
        out_shape=(vmem(eddy_shape, f32), vmem(transport_shape, f32)),
        in_specs=[pl.BlockSpec(memory_space=pltpu.HBM)] * 5,
        out_specs=(pl.BlockSpec(memory_space=vmem), pl.BlockSpec(memory_space=vmem)),
        scratch_shapes=[
            vmem((3, rows, columns), i32),
            vmem((rows + SUB, columns), f32),
            vmem((planes, rows, columns), f32),
            vmem((planes, rows + SUB, columns), f32),
            vmem((levels, rows, columns), f32),
            vmem((blocks, fields * SUB, LANES), f32),
            vmem((planes + SUB, LANES), f32),
            vmem((planes + SUB, LANES), f32),
            vmem((parities, slots, packed, LANES), f32),
            vmem((slots, packed, LANES), f32),
            vmem((slots, packed, LANES), f32),
            vmem((chips, packed, LANES), f32),
            vmem((slots, SUB, LANES), f32),
            vmem((chips, slots, SUB, LANES), f32),
            vmem((parities, slots, SUB, LANES), f32),
            vmem((SUB, LANES), f32),
            vmem((lon_devices, SUB, LANES), f32),
            vmem((2 * SUB, LANES), f32),
            vmem((lon_devices, 2 * SUB, LANES), f32),
            vmem((SUB, LANES), f32),
            vmem((2 * SUB, LANES), f32),
            dma,
            dma,
            dma((GROUPS,)),
            dma,
            dma,
            dma,
            dma((GROUPS,)),
            dma,
            dma,
            dma,
            dma,
            dma,
            dma,
            dma,
            dma,
            dma,
            dma,
        ],
        compiler_params=pltpu.CompilerParams(
            collective_id=0, has_side_effects=True, vmem_limit_bytes=62 * 1024 * 1024
        ),
        name="heat_transport",
    )(
        poleward_flow.reshape(planes, rows, columns),
        potential_warmth.reshape(planes, rows, columns),
        water_profile_flag,
        floor_count,
        catchment_label_for_site,
    )
    eddy_temp, transport = pl.pallas_call(
        store,
        out_shape=(
            jax.ShapeDtypeStruct(eddy_shape, f32), jax.ShapeDtypeStruct(transport_shape, f32)
        ),
        in_specs=[pl.BlockSpec(memory_space=vmem)] * 2,
        out_specs=(pl.BlockSpec(memory_space=pltpu.HBM), pl.BlockSpec(memory_space=pltpu.HBM)),
        scratch_shapes=[dma((2,))],
        name="store_results",
    )(
        pltpu.with_memory_space_constraint(eddy_temp, vmem),
        pltpu.with_memory_space_constraint(transport, vmem),
    )
    return eddy_temp, jnp.transpose(transport, (0, 3, 1, 2))


def solution(mesh):
    return jax.shard_map(
        functools.partial(shards, mesh.shape["lat"], mesh.shape["lon"]),
        mesh=mesh,
        in_specs=(
            P(None, None, "lat", "lon"),
            P(None, None, "lat", "lon"),
            P("lat", "lon"),
            P("lat", "lon"),
            P("lat", "lon"),
        ),
        out_specs=(P(None, "lat", "lon"), P(None, None, None, ("lat", "lon"))),
        check_vma=False,
    )
```

```python
import functools
import math

import jax
import jax.numpy as jnp
from jax import lax
from jax.experimental import pallas as pl
from jax.experimental.pallas import tpu as pltpu
from jax.sharding import PartitionSpec as P

BASINS = 10
MESH = pl.DeviceIdType.MESH
SUB = 8
LANES = 128
GROUPS = 2


def kernel(
    lat_devices, lon_devices, snapshots, levels, share_rows,
    flow_hbm, warmth_hbm, flag_hbm, floor_hbm, label_hbm,
    eddy_ref, transport_ref,
    columns, depth, flow, warmth, average, dots, mean_dots, members,
    halo_out, halo_in, stats, pair_stats, chip_stats, received, sums, pair_sums, chip_sums, peer_sums, all_sums,
    edge_sums, peer_edge, edge_stats, peer_edge_stats, edge_total, edge_stats_total,
    load_first, load_warmth, load_flow, halo_send, halo_recv,
    sums_pair_send, sums_pair_recv, pair_send, pair_recv, stat_send, stat_recv, sum_send, sum_recv, share_send, share_recv,
    edge_send, edge_recv, edge_stat_send, edge_stat_recv,
):
    rows = flow.shape[1]
    blocks = rows // SUB
    last = blocks - 1
    half_blocks = blocks // GROUPS
    label_ref = columns.at[2]
    owners = SUB // share_rows
    planes = snapshots * levels
    parities, slots, packed = stats.shape[:3]
    group_slots = slots // GROUPS
    fields = dots.shape[1] // SUB
    used = BASINS * SUB
    chips = lon_devices // 2
    lat = lax.axis_index("lat")
    me = lax.axis_index("lon")
    core = lax.rem(me, 2)
    chip = me // 2
    mine = core if parities == 2 else 0
    theirs = 1 - core if parities == 2 else 0
    partner = (lat, me + 1 - 2 * core)
    own_slot = me // (owners * parities)
    scaling = 1.0 / math.sqrt(LANES * lon_devices)
    has_next = lat < lat_devices - 1

    def window(b):
        return pl.ds(b * SUB, SUB)

    def flow_copy(b):
        at = window(b)
        return pltpu.make_async_copy(
            flow_hbm.at[:, at, :], flow.at[:, at, :], load_flow.at[b // half_blocks]
        )

    def warmth_copy(b):
        at = window(b)
        sem = load_warmth if b else load_first
        return pltpu.make_async_copy(warmth_hbm.at[:, at, :], warmth.at[:, at, :], sem)

    def await_bytes(ref, sem):
        pltpu.make_async_copy(ref, ref, sem).wait()

    def await_flow(g):
        await_bytes(flow.at[:, pl.ds(0, half_blocks * SUB), :], load_flow.at[g])

    for n, column in enumerate((flag_hbm, floor_hbm, label_hbm)):
        pltpu.make_async_copy(column, columns.at[n], load_first).start()
    for b in range(blocks):
        warmth_copy(b).start()
    for b in range(blocks):
        flow_copy(b).start()

    barrier = pltpu.get_barrier_semaphore()

    def greet(d, carry):
        pl.semaphore_signal(
            barrier, inc=1, device_id=(lat, lax.rem(me + d, lon_devices)), device_id_type=MESH
        )
        return carry

    @pl.when(has_next)
    def _():
        pl.semaphore_signal(barrier, inc=1, device_id=(lat + 1, me), device_id_type=MESH)

    lax.fori_loop(1, lon_devices, greet, 0)

    halo_copy = pltpu.make_async_remote_copy(
        src_ref=halo_out, dst_ref=halo_in, send_sem=halo_send, recv_sem=halo_recv,
        device_id=(jnp.maximum(lat - 1, 0), me), device_id_type=MESH,
    )

    def group(g):
        return pl.ds(g * group_slots, group_slots)

    def pair_copy(g):
        return pltpu.make_async_remote_copy(
            src_ref=stats.at[theirs, group(g)], dst_ref=pair_stats.at[group(g)],
            send_sem=pair_send, recv_sem=pair_recv.at[g],
            device_id=partner, device_id_type=MESH,
        )

    sums_pair_copy = pltpu.make_async_remote_copy(
        src_ref=sums.at[theirs], dst_ref=pair_sums,
        send_sem=sums_pair_send, recv_sem=sums_pair_recv, device_id=partner, device_id_type=MESH,
    )

    def sum_copy(to, source):
        return pltpu.make_async_remote_copy(
            src_ref=chip_sums, dst_ref=peer_sums.at[source],
            send_sem=sum_send, recv_sem=sum_recv,
            device_id=(lat, 2 * to + core), device_id_type=MESH,
        )

    def stat_slot(to):
        return (2 * to + core) // (owners * parities)

    def stat_copy(to, source):
        return pltpu.make_async_remote_copy(
            src_ref=chip_stats.at[stat_slot(to)], dst_ref=received.at[source],
            send_sem=stat_send, recv_sem=stat_recv,
            device_id=(lat, 2 * to + core), device_id_type=MESH,
        )

    share_copy = pltpu.make_async_remote_copy(
        src_ref=all_sums.at[mine], dst_ref=all_sums.at[mine],
        send_sem=share_send, recv_sem=share_recv, device_id=partner, device_id_type=MESH,
    )

    def edge_copy(to, source):
        return pltpu.make_async_remote_copy(
            src_ref=edge_sums, dst_ref=peer_edge.at[source],
            send_sem=edge_send, recv_sem=edge_recv,
            device_id=(lat, to), device_id_type=MESH,
        )

    def edge_stat_copy(source):
        return pltpu.make_async_remote_copy(
            src_ref=edge_stats, dst_ref=peer_edge_stats.at[source],
            send_sem=edge_stat_send, recv_sem=edge_stat_recv,
            device_id=(lat, lon_devices - 1), device_id_type=MESH,
        )

    def each_chip(action):
        def step(d, carry):
            action(lax.rem(chip + d, chips))
            return carry

        lax.fori_loop(1, chips, step, 0)

    def each_peer(action):
        def step(d, carry):
            action(lax.rem(me + d, lon_devices))
            return carry

        lax.fori_loop(1, lon_devices, step, 0)

    sub = lax.broadcasted_iota(jnp.int32, (SUB, LANES), 0)
    level = lax.broadcasted_iota(jnp.int32, (levels, SUB, LANES), 0).astype(jnp.float32)

    def next_row(here, after):
        first = lax.broadcasted_iota(jnp.int32, here.shape, here.ndim - 2) == 0
        return pltpu.roll(jnp.where(first, after, here), SUB - 1, here.ndim - 2)

    def both_halves(x):
        return x + pltpu.roll(x, levels, 0)

    def wet_cells(b):
        here = depth[window(b), :]
        limit = jnp.minimum(here, next_row(here, depth[window(b + 1), :]))
        return (level < limit[None]).astype(jnp.float32)

    def split_dot(values, member):
        high = values.astype(jnp.bfloat16)
        low = (values - high.astype(jnp.float32)).astype(jnp.bfloat16)
        return lax.dot_general(
            jnp.concatenate([high, low], axis=1), jnp.concatenate([member, member], axis=1),
            (((1,), (1,)), ((), ())), preferred_element_type=jnp.float32,
        )

    def by_row(ref, count):
        row_of = lax.rem(lax.broadcasted_iota(jnp.int32, (count, LANES), 1), SUB)
        zonal = ref[pl.ds(0, count, stride=SUB), :]
        for j in range(1, SUB):
            zonal = jnp.where(row_of == j, ref[pl.ds(j, count, stride=SUB), :], zonal)
        return zonal

    def block_means(b):
        at = window(b)
        wet = wet_cells(b)
        here = jnp.sum(warmth[:, at, :].reshape(snapshots, levels, SUB, LANES), axis=0)
        after = jnp.sum(
            warmth[:, window(b + 1), :].reshape(snapshots, levels, SUB, LANES)[:, :, :1], axis=0
        )
        mean_warmth = (here + next_row(here, after)) * (0.5 / snapshots)
        average[:, at, :] = mean_warmth
        labels = label_ref[at, :]
        member = jnp.concatenate(
            [(labels == n).astype(jnp.float32) for n in range(LANES // SUB)], axis=0
        ).astype(jnp.bfloat16)
        members[b] = member
        values = jnp.concatenate([mean_warmth * wet, wet], axis=0).reshape(-1, LANES)
        mean_dots[b] = split_dot(values, member)
        sums[b % parities, b // parities] = by_row(mean_dots.at[b], 2 * levels)

    def block_stats(b):
        at = window(b)
        wet = wet_cells(b)
        velocity = flow[:, at, :].reshape(snapshots, levels, SUB, LANES)
        here = warmth[:, at, :]
        point = (0.5 * (here + next_row(here, warmth[:, window(b + 1), :]))).reshape(
            snapshots, levels, SUB, LANES
        )
        mean_warmth = average[:, at, :]
        mean_velocity = jnp.sum(velocity, axis=0) * (1.0 / snapshots)
        cross = jnp.sum((velocity - mean_velocity) * (point - mean_warmth), axis=0) * (1.0 / snapshots)
        values = jnp.concatenate(
            [
                (point * wet[None]).reshape(planes, SUB, LANES),
                wet,
                wet,
                (velocity * wet[None]).reshape(planes, SUB, LANES),
                mean_velocity * mean_warmth * wet,
                cross * wet,
            ],
            axis=0,
        ).reshape(-1, LANES)
        dots[b] = split_dot(values, members[b])
        zonal = by_row(dots.at[b], fields)
        half = packed // 2
        rest = zonal[packed:]
        spare = lax.broadcasted_iota(jnp.int32, (half, LANES), 1) >= used
        stats[b % parities, b // parities] = jnp.concatenate(
            [
                jnp.where(spare, pltpu.roll(rest, used, 1), zonal[:half]),
                jnp.where(spare, pltpu.roll(rest, 2 * used - LANES, 1), zonal[half:packed]),
            ],
            axis=0,
        )

    def sums_of(zonal):
        warmth_sum = both_halves(jnp.sum(zonal[:planes].reshape(planes // SUB, SUB, LANES), axis=0))
        return jnp.where(sub < levels, warmth_sum * (1.0 / snapshots), zonal[planes : planes + SUB])

    def add_pair(g):
        pair_copy(g).wait_recv()
        for s in range(g * group_slots, (g + 1) * group_slots):
            chip_stats[s] = stats[mine, s] + pair_stats[s]

    def send_sums():
        sums_pair_copy.wait_recv()
        chip_sums[...] = sums[mine] + pair_sums[...]
        each_chip(lambda to: sum_copy(to, chip).start())

    def send_group_stats(g):
        def send_stats(to):
            @pl.when(stat_slot(to) // group_slots == g)
            def _():
                stat_copy(to, chip).start()

        each_chip(send_stats)

    await_bytes(columns, load_first)
    await_bytes(warmth.at[:, window(0), :], load_first)
    depth[pl.ds(0, rows), :] = (columns[0] * columns[1]).astype(jnp.float32)
    depth[pl.ds(rows, SUB), :] = jnp.zeros((SUB, LANES), jnp.float32)
    warmth[:, rows, :] = jnp.zeros((planes, LANES), jnp.float32)
    halo_out[pl.ds(0, planes), :] = warmth[:, 0, :]
    halo_out[pl.ds(planes, SUB), :] = depth[pl.ds(0, SUB), :]

    pl.semaphore_wait(barrier, lon_devices - 1 + (lat > 0).astype(jnp.int32))

    @pl.when(lat > 0)
    def _():
        halo_copy.start()

    await_bytes(warmth.at[:, pl.ds(0, last * SUB), :], load_warmth)
    for b in range(blocks):
        block_means(b)
    sums_pair_copy.start()
    await_flow(0)
    for b in range(half_blocks):
        block_stats(b)
    pair_copy(0).start()
    @pl.when(core == 0)
    def _():
        send_sums()

    await_flow(1)
    for b in range(half_blocks, blocks):
        block_stats(b)
    pair_copy(1).start()

    @pl.when(core == 1)
    def _():
        send_sums()

    add_pair(0)
    send_group_stats(0)

    lanes = lax.broadcasted_iota(jnp.int32, (SUB, LANES), 1)
    edge_total[...] = jnp.zeros((SUB, LANES), jnp.float32)

    @pl.when(has_next)
    def _():
        at = rows - 1
        column = lax.broadcasted_iota(jnp.int32, (LANES, LANES), 0)
        chosen = jnp.logical_and(
            lax.rem(column, SUB) == SUB - 1, label_ref[pl.ds(at, 1), :] == column // SUB
        )
        member = chosen.astype(jnp.float32).astype(jnp.bfloat16)
        velocity = flow[:, at, :].reshape(planes // SUB, SUB, LANES)
        mean_velocity = both_halves(jnp.sum(velocity, axis=0)) * (1.0 / snapshots)
        here = warmth[:, at, :]
        halo_copy.wait_recv()
        limit = jnp.minimum(depth[pl.ds(at, 1), :], halo_in[pl.ds(planes, 1), :])
        wet = (lax.rem(sub, levels).astype(jnp.float32) < limit).astype(jnp.float32)
        point = (0.5 * (here + halo_in[pl.ds(0, planes), :])).reshape(planes // SUB, SUB, LANES)
        mean_warmth = both_halves(jnp.sum(point, axis=0)) * (1.0 / snapshots)
        cross = both_halves(
            jnp.sum((velocity - mean_velocity) * (point - mean_warmth), axis=0)
        ) * (1.0 / snapshots)
        average[:, at, :] = mean_warmth[:levels]
        depth[pl.ds(rows, SUB), :] = halo_in[pl.ds(planes, SUB), :]
        values = jnp.concatenate(
            [
                (point * wet).reshape(planes, LANES),
                wet,
                (velocity * wet).reshape(planes, LANES),
                jnp.where(sub < levels, mean_velocity * mean_warmth, cross) * wet,
            ],
            axis=0,
        )
        zonal = split_dot(values, member)
        edge_sums[...] = sums_of(zonal)
        each_peer(lambda to: edge_copy(to, me).start())
        parts = [zonal[SUB * n : SUB * (n + 1)] for n in range(fields // SUB)]
        first = parts[0]
        for n in range(1, SUB):
            first = first + pltpu.roll(parts[n], LANES - n, 1)
        second = parts[SUB]
        for n in range(SUB + 1, fields // SUB):
            second = second + pltpu.roll(parts[n], LANES - (n - SUB), 1)
        edge_stats[...] = jnp.concatenate([first, second], axis=0)

        @pl.when(me < lon_devices - 1)
        def _():
            edge_stat_copy(me).start()

    add_pair(1)
    send_group_stats(1)

    def block_eddy(b, block_sums):
        at = pl.ds(b * SUB, SUB)
        wet = wet_cells(b)
        index = label_ref[at, :] * SUB + sub
        bar = block_sums / jnp.maximum(pltpu.roll(block_sums, levels, 0), 1.0)
        for k in range(levels):
            cells = jnp.take_along_axis(
                jnp.broadcast_to(bar[k : k + 1], (SUB, LANES)), index, axis=1
            )
            eddy_ref[k, at, :] = wet[k] * (average[k, at, :] - cells)

    def add_sums(d, total):
        source = lax.rem(chip + chips - d, chips)
        return total + peer_sums[pl.ds(source, 1)][0]

    await_bytes(peer_sums.at[pl.ds(0, chips - 1)], sum_recv)
    all_sums[mine] = lax.fori_loop(1, chips, add_sums, chip_sums[...], unroll=chips <= SUB)
    if parities == 2:
        share_copy.start()

    def write_transport(total, early):
        half = packed // 2
        lane = lax.broadcasted_iota(jnp.int32, (half, LANES), 1)
        total = jnp.concatenate(
            [
                total,
                jnp.where(
                    lane < LANES - used,
                    pltpu.roll(total[:half], LANES - used, 1),
                    pltpu.roll(total[half:], 2 * LANES - 2 * used, 1),
                ),
            ],
            axis=0,
        )
        extra = None if early else edge_stats_total[...]
        edge_lane = lax.rem(lanes, SUB) == SUB - 1
        pieces = []
        for n in range(fields // SUB):
            piece = total[SUB * n : SUB * (n + 1)]
            if extra is not None:
                part = extra[:SUB] if n < SUB else extra[SUB:]
                if n % SUB:
                    part = pltpu.roll(part, n % SUB, 1)
                piece = piece + jnp.where(edge_lane, part, 0.0)
            pieces.append(piece)
        shape = (planes // SUB, SUB, LANES)
        per = planes // SUB
        count = pieces[per]
        divisor = jnp.maximum(count, 1.0)
        means_t = jnp.stack(pieces[:per]) / divisor
        means_v = jnp.stack(pieces[per + 1 : 2 * per + 1]) / divisor
        bar_v = both_halves(jnp.sum(means_v, axis=0)) * (1.0 / snapshots)
        bar_t = both_halves(jnp.sum(means_t, axis=0)) * (1.0 / snapshots)
        swing = both_halves(jnp.sum((means_v - bar_v) * (means_t - bar_t), axis=0)) * (1.0 / snapshots)
        upper = jnp.where(sub < levels, scaling * count * bar_v * bar_t, scaling * count * swing)
        lower = scaling * pieces[2 * per + 1] - upper
        if owners > 1:
            shift = LANES - lax.rem(me, owners) * share_rows
            upper = pltpu.roll(upper, shift, 1)
            lower = pltpu.roll(lower, shift, 1)
        spread = lax.rem(lanes * SUB + sub, LANES)
        for c, part in enumerate((upper, lower, upper, lower)):
            for k in range(levels):
                row = c // 2 * levels + k
                table = jnp.take_along_axis(
                    jnp.broadcast_to(part[row : row + 1], (SUB, LANES)), spread, axis=1
                )
                transport_ref[c, k] = table[:share_rows, :BASINS]

    def add_received(d, total):
        source = lax.rem(chip + chips - d, chips)
        return total + received[pl.ds(source, 1)][0]

    if parities == 2:
        share_copy.wait_recv()
    for b in range(last):
        block_eddy(b, all_sums[b % parities, b // parities])

    await_bytes(received.at[pl.ds(0, chips - 1)], stat_recv)
    total = lax.fori_loop(
        1, chips, add_received, chip_stats[pl.ds(own_slot, 1)][0], unroll=chips <= SUB
    )
    late = jnp.logical_and(has_next, me == lon_devices - 1)

    @pl.when(jnp.logical_not(late))
    def _():
        write_transport(total, True)

    @pl.when(has_next)
    def _():
        def add_edge(d, total):
            source = lax.rem(me + lon_devices - d, lon_devices)
            return total + peer_edge[pl.ds(source, 1)][0]

        await_bytes(peer_edge.at[pl.ds(0, lon_devices - 1)], edge_recv)
        edge_total[...] = lax.fori_loop(
            1, lon_devices, add_edge, edge_sums[...], unroll=lon_devices <= SUB
        )

    block_eddy(last, all_sums[last % parities, last // parities] + edge_total[...])
    @pl.when(late)
    def _():
        def add_edge_stats(d, total):
            source = lax.rem(me + lon_devices - d, lon_devices)
            return total + peer_edge_stats[pl.ds(source, 1)][0]

        await_bytes(peer_edge_stats.at[pl.ds(0, lon_devices - 1)], edge_stat_recv)
        edge_stats_total[...] = lax.fori_loop(
            1, lon_devices, add_edge_stats, edge_stats[...], unroll=lon_devices <= SUB
        )
        write_transport(total, False)

    @pl.when(lat > 0)
    def _():
        halo_copy.wait_send()

    sums_pair_copy.wait_send()
    await_bytes(pair_stats, pair_send)
    await_bytes(peer_sums.at[pl.ds(0, chips - 1)], sum_send)
    await_bytes(received.at[pl.ds(0, chips - 1)], stat_send)
    if parities == 2:
        share_copy.wait_send()

    @pl.when(has_next)
    def _():
        await_bytes(peer_edge.at[pl.ds(0, lon_devices - 1)], edge_send)

        @pl.when(me < lon_devices - 1)
        def _():
            edge_stat_copy(me).wait_send()


def store(eddy_ref, transport_ref, eddy_hbm, transport_hbm, sems):
    copies = (
        pltpu.make_async_copy(eddy_ref, eddy_hbm, sems.at[0]),
        pltpu.make_async_copy(transport_ref, transport_hbm, sems.at[1]),
    )
    for copy in copies:
        copy.start()
    for copy in copies:
        copy.wait()


def shards(
    lat_devices, lon_devices,
    poleward_flow, potential_warmth, water_profile_flag, floor_count, catchment_label_for_site,
):
    snapshots, levels, rows, columns = poleward_flow.shape
    share_rows = rows // lon_devices
    blocks = rows // SUB
    planes = snapshots * levels
    fields = 2 * planes + 4 * levels
    packed = fields * 2 // 3
    chips = lon_devices // 2
    parities = 2 if share_rows == SUB else 1
    slots = blocks // parities
    f32, i32, vmem, dma = jnp.float32, jnp.int32, pltpu.VMEM, pltpu.SemaphoreType.DMA
    eddy_shape = (levels, rows, columns)
    transport_shape = (4, levels, share_rows, BASINS)
    eddy_temp, transport = pl.pallas_call(
        functools.partial(kernel, lat_devices, lon_devices, snapshots, levels, share_rows),
        out_shape=(vmem(eddy_shape, f32), vmem(transport_shape, f32)),
        in_specs=[pl.BlockSpec(memory_space=pltpu.HBM)] * 5,
        out_specs=(pl.BlockSpec(memory_space=vmem), pl.BlockSpec(memory_space=vmem)),
        scratch_shapes=[
            vmem((3, rows, columns), i32),
            vmem((rows + SUB, columns), f32),
            vmem((planes, rows, columns), f32),
            vmem((planes, rows + SUB, columns), f32),
            vmem((levels, rows, columns), f32),
            vmem((blocks, fields * SUB, LANES), f32),
            vmem((blocks, 2 * levels * SUB, LANES), f32),
            vmem((blocks, LANES, LANES), jnp.bfloat16),
            vmem((planes + SUB, LANES), f32),
            vmem((planes + SUB, LANES), f32),
            vmem((parities, slots, packed, LANES), f32),
            vmem((slots, packed, LANES), f32),
            vmem((slots, packed, LANES), f32),
            vmem((chips, packed, LANES), f32),
            vmem((parities, slots, SUB, LANES), f32),
            vmem((slots, SUB, LANES), f32),
            vmem((slots, SUB, LANES), f32),
            vmem((chips, slots, SUB, LANES), f32),
            vmem((parities, slots, SUB, LANES), f32),
            vmem((SUB, LANES), f32),
            vmem((lon_devices, SUB, LANES), f32),
            vmem((2 * SUB, LANES), f32),
            vmem((lon_devices, 2 * SUB, LANES), f32),
            vmem((SUB, LANES), f32),
            vmem((2 * SUB, LANES), f32),
            dma,
            dma,
            dma((GROUPS,)),
            dma,
            dma,
            dma,
            dma,
            dma,
            dma((GROUPS,)),
            dma,
            dma,
            dma,
            dma,
            dma,
            dma,
            dma,
            dma,
            dma,
            dma,
        ],
        compiler_params=pltpu.CompilerParams(
            collective_id=0, has_side_effects=True, vmem_limit_bytes=62 * 1024 * 1024
        ),
        name="heat_transport",
    )(
        poleward_flow.reshape(planes, rows, columns),
        potential_warmth.reshape(planes, rows, columns),
        water_profile_flag,
        floor_count,
        catchment_label_for_site,
    )
    eddy_temp, transport = pl.pallas_call(
        store,
        out_shape=(
            jax.ShapeDtypeStruct(eddy_shape, f32), jax.ShapeDtypeStruct(transport_shape, f32)
        ),
        in_specs=[pl.BlockSpec(memory_space=vmem)] * 2,
        out_specs=(pl.BlockSpec(memory_space=pltpu.HBM), pl.BlockSpec(memory_space=pltpu.HBM)),
        scratch_shapes=[dma((2,))],
        name="store_results",
    )(
        pltpu.with_memory_space_constraint(eddy_temp, vmem),
        pltpu.with_memory_space_constraint(transport, vmem),
    )
    return eddy_temp, jnp.transpose(transport, (0, 3, 1, 2))


def solution(mesh):
    return jax.shard_map(
        functools.partial(shards, mesh.shape["lat"], mesh.shape["lon"]),
        mesh=mesh,
        in_specs=(
            P(None, None, "lat", "lon"),
            P(None, None, "lat", "lon"),
            P("lat", "lon"),
            P("lat", "lon"),
            P("lat", "lon"),
        ),
        out_specs=(P(None, "lat", "lon"), P(None, None, None, ("lat", "lon"))),
        check_vma=False,
    )
```

```python
import functools
import math

import jax
import jax.numpy as jnp
from jax import lax
from jax.experimental import pallas as pl
from jax.experimental.pallas import tpu as pltpu
from jax.sharding import PartitionSpec as P

BASINS = 10
MESH = pl.DeviceIdType.MESH
SUB = 8
LANES = 128
GROUPS = 2


def kernel(
    lat_devices, lon_devices, snapshots, levels, share_rows,
    flow_hbm, warmth_hbm, flag_hbm, floor_hbm, label_hbm,
    eddy_ref, transport_ref,
    columns, depth, flow, warmth, average, dots, mean_dots, members,
    halo_out, halo_in, stats, pair_stats, chip_stats, received, sums, pair_sums, chip_sums, peer_sums, all_sums,
    edge_sums, peer_edge, edge_stats, peer_edge_stats, edge_total, edge_stats_total,
    load_first, load_warmth, load_flow, halo_send, halo_recv,
    sums_pair_send, sums_pair_recv, pair_send, pair_recv, stat_send, stat_recv, sum_send, sum_recv, share_send, share_recv,
    edge_send, edge_recv, edge_stat_send, edge_stat_recv,
):
    rows = flow.shape[1]
    blocks = rows // SUB
    last = blocks - 1
    half_blocks = blocks // GROUPS
    label_ref = columns.at[2]
    owners = SUB // share_rows
    planes = snapshots * levels
    parities, slots, packed = stats.shape[:3]
    group_slots = slots // GROUPS
    fields = dots.shape[1] // SUB
    used = BASINS * SUB
    chips = lon_devices // 2
    lat = lax.axis_index("lat")
    me = lax.axis_index("lon")
    core = lax.rem(me, 2)
    chip = me // 2
    mine = core if parities == 2 else 0
    theirs = 1 - core if parities == 2 else 0
    partner = (lat, me + 1 - 2 * core)
    own_slot = me // (owners * parities)
    scaling = 1.0 / math.sqrt(LANES * lon_devices)
    has_next = lat < lat_devices - 1

    def window(b):
        return pl.ds(b * SUB, SUB)

    def flow_copy(b):
        at = window(b)
        return pltpu.make_async_copy(
            flow_hbm.at[:, at, :], flow.at[:, at, :], load_flow.at[b // half_blocks]
        )

    def warmth_copy(b):
        at = window(b)
        sem = load_warmth if b else load_first
        return pltpu.make_async_copy(warmth_hbm.at[:, at, :], warmth.at[:, at, :], sem)

    def await_bytes(ref, sem):
        pltpu.make_async_copy(ref, ref, sem).wait()

    def await_flow(g):
        await_bytes(flow.at[:, pl.ds(0, half_blocks * SUB), :], load_flow.at[g])

    for n, column in enumerate((flag_hbm, floor_hbm, label_hbm)):
        pltpu.make_async_copy(column, columns.at[n], load_first).start()
    for b in range(blocks):
        warmth_copy(b).start()
    barrier = pltpu.get_barrier_semaphore()

    def greet(d, carry):
        pl.semaphore_signal(
            barrier, inc=1, device_id=(lat, lax.rem(me + d, lon_devices)), device_id_type=MESH
        )
        return carry

    @pl.when(has_next)
    def _():
        pl.semaphore_signal(barrier, inc=1, device_id=(lat + 1, me), device_id_type=MESH)

    lax.fori_loop(1, lon_devices, greet, 0)
    for b in range(blocks):
        flow_copy(b).start()

    halo_copy = pltpu.make_async_remote_copy(
        src_ref=halo_out, dst_ref=halo_in, send_sem=halo_send, recv_sem=halo_recv,
        device_id=(jnp.maximum(lat - 1, 0), me), device_id_type=MESH,
    )

    def group(g):
        return pl.ds(g * group_slots, group_slots)

    def pair_copy(g):
        return pltpu.make_async_remote_copy(
            src_ref=stats.at[theirs, group(g)], dst_ref=pair_stats.at[group(g)],
            send_sem=pair_send, recv_sem=pair_recv.at[g],
            device_id=partner, device_id_type=MESH,
        )

    sums_pair_copy = pltpu.make_async_remote_copy(
        src_ref=sums.at[theirs], dst_ref=pair_sums,
        send_sem=sums_pair_send, recv_sem=sums_pair_recv, device_id=partner, device_id_type=MESH,
    )

    def sum_copy(to, source):
        return pltpu.make_async_remote_copy(
            src_ref=chip_sums, dst_ref=peer_sums.at[source],
            send_sem=sum_send, recv_sem=sum_recv,
            device_id=(lat, 2 * to + core), device_id_type=MESH,
        )

    def stat_slot(to):
        return (2 * to + core) // (owners * parities)

    def stat_copy(to, source):
        return pltpu.make_async_remote_copy(
            src_ref=chip_stats.at[stat_slot(to)], dst_ref=received.at[source],
            send_sem=stat_send, recv_sem=stat_recv,
            device_id=(lat, 2 * to + core), device_id_type=MESH,
        )

    share_copy = pltpu.make_async_remote_copy(
        src_ref=all_sums.at[mine], dst_ref=all_sums.at[mine],
        send_sem=share_send, recv_sem=share_recv, device_id=partner, device_id_type=MESH,
    )

    def edge_copy(to, source):
        return pltpu.make_async_remote_copy(
            src_ref=edge_sums, dst_ref=peer_edge.at[source],
            send_sem=edge_send, recv_sem=edge_recv,
            device_id=(lat, to), device_id_type=MESH,
        )

    def edge_stat_copy(source):
        return pltpu.make_async_remote_copy(
            src_ref=edge_stats, dst_ref=peer_edge_stats.at[source],
            send_sem=edge_stat_send, recv_sem=edge_stat_recv,
            device_id=(lat, lon_devices - 1), device_id_type=MESH,
        )

    def each_chip(action):
        def step(d, carry):
            action(lax.rem(chip + d, chips))
            return carry

        lax.fori_loop(1, chips, step, 0)

    def each_peer(action):
        def step(d, carry):
            action(lax.rem(me + d, lon_devices))
            return carry

        lax.fori_loop(1, lon_devices, step, 0)

    sub = lax.broadcasted_iota(jnp.int32, (SUB, LANES), 0)
    level = lax.broadcasted_iota(jnp.int32, (levels, SUB, LANES), 0).astype(jnp.float32)

    def next_row(here, after):
        first = lax.broadcasted_iota(jnp.int32, here.shape, here.ndim - 2) == 0
        return pltpu.roll(jnp.where(first, after, here), SUB - 1, here.ndim - 2)

    def both_halves(x):
        return x + pltpu.roll(x, levels, 0)

    def wet_cells(b):
        here = depth[window(b), :]
        limit = jnp.minimum(here, next_row(here, depth[window(b + 1), :]))
        return (level < limit[None]).astype(jnp.float32)

    def split_dot(values, member):
        high = values.astype(jnp.bfloat16)
        low = (values - high.astype(jnp.float32)).astype(jnp.bfloat16)
        return lax.dot_general(
            jnp.concatenate([high, low], axis=1), jnp.concatenate([member, member], axis=1),
            (((1,), (1,)), ((), ())), preferred_element_type=jnp.float32,
        )

    def by_row(ref, count):
        row_of = lax.rem(lax.broadcasted_iota(jnp.int32, (count, LANES), 1), SUB)
        zonal = ref[pl.ds(0, count, stride=SUB), :]
        for j in range(1, SUB):
            zonal = jnp.where(row_of == j, ref[pl.ds(j, count, stride=SUB), :], zonal)
        return zonal

    def block_means(b):
        at = window(b)
        wet = wet_cells(b)
        here = jnp.sum(warmth[:, at, :].reshape(snapshots, levels, SUB, LANES), axis=0)
        after = jnp.sum(
            warmth[:, window(b + 1), :].reshape(snapshots, levels, SUB, LANES)[:, :, :1], axis=0
        )
        mean_warmth = (here + next_row(here, after)) * (0.5 / snapshots)
        average[:, at, :] = mean_warmth
        labels = label_ref[at, :]
        member = jnp.concatenate(
            [(labels == n).astype(jnp.float32) for n in range(LANES // SUB)], axis=0
        ).astype(jnp.bfloat16)
        members[b] = member
        values = jnp.concatenate([mean_warmth * wet, wet], axis=0).reshape(-1, LANES)
        mean_dots[b] = split_dot(values, member)
        sums[b % parities, b // parities] = by_row(mean_dots.at[b], 2 * levels)

    def block_stats(b):
        at = window(b)
        wet = wet_cells(b)
        velocity = flow[:, at, :].reshape(snapshots, levels, SUB, LANES)
        here = warmth[:, at, :]
        point = (0.5 * (here + next_row(here, warmth[:, window(b + 1), :]))).reshape(
            snapshots, levels, SUB, LANES
        )
        mean_warmth = average[:, at, :]
        mean_velocity = jnp.sum(velocity, axis=0) * (1.0 / snapshots)
        cross = jnp.sum((velocity - mean_velocity) * (point - mean_warmth), axis=0) * (1.0 / snapshots)
        values = jnp.concatenate(
            [
                (point * wet[None]).reshape(planes, SUB, LANES),
                wet,
                wet,
                (velocity * wet[None]).reshape(planes, SUB, LANES),
                mean_velocity * mean_warmth * wet,
                cross * wet,
            ],
            axis=0,
        ).reshape(-1, LANES)
        dots[b] = split_dot(values, members[b])
        zonal = by_row(dots.at[b], fields)
        half = packed // 2
        rest = zonal[packed:]
        spare = lax.broadcasted_iota(jnp.int32, (half, LANES), 1) >= used
        stats[b % parities, b // parities] = jnp.concatenate(
            [
                jnp.where(spare, pltpu.roll(rest, used, 1), zonal[:half]),
                jnp.where(spare, pltpu.roll(rest, 2 * used - LANES, 1), zonal[half:packed]),
            ],
            axis=0,
        )

    def sums_of(zonal):
        warmth_sum = both_halves(jnp.sum(zonal[:planes].reshape(planes // SUB, SUB, LANES), axis=0))
        return jnp.where(sub < levels, warmth_sum * (1.0 / snapshots), zonal[planes : planes + SUB])

    def add_pair(g):
        pair_copy(g).wait_recv()
        for s in range(g * group_slots, (g + 1) * group_slots):
            chip_stats[s] = stats[mine, s] + pair_stats[s]

    def send_sums():
        sums_pair_copy.wait_recv()
        chip_sums[...] = sums[mine] + pair_sums[...]
        each_chip(lambda to: sum_copy(to, chip).start())

    def send_group_stats(g):
        def send_stats(to):
            @pl.when(stat_slot(to) // group_slots == g)
            def _():
                stat_copy(to, chip).start()

        each_chip(send_stats)

    await_bytes(columns, load_first)
    await_bytes(warmth.at[:, window(0), :], load_first)
    depth[pl.ds(0, rows), :] = (columns[0] * columns[1]).astype(jnp.float32)
    depth[pl.ds(rows, SUB), :] = jnp.zeros((SUB, LANES), jnp.float32)
    warmth[:, rows, :] = jnp.zeros((planes, LANES), jnp.float32)
    halo_out[pl.ds(0, planes), :] = warmth[:, 0, :]
    halo_out[pl.ds(planes, SUB), :] = depth[pl.ds(0, SUB), :]

    pl.semaphore_wait(barrier, lon_devices - 1 + (lat > 0).astype(jnp.int32))

    @pl.when(lat > 0)
    def _():
        halo_copy.start()

    await_bytes(warmth.at[:, pl.ds(0, last * SUB), :], load_warmth)
    for b in range(blocks):
        block_means(b)
    sums_pair_copy.start()
    await_flow(0)
    for b in range(half_blocks):
        block_stats(b)
    pair_copy(0).start()
    @pl.when(core == 0)
    def _():
        send_sums()

    await_flow(1)
    for b in range(half_blocks, blocks):
        block_stats(b)
    pair_copy(1).start()

    @pl.when(core == 1)
    def _():
        send_sums()

    add_pair(0)
    send_group_stats(0)

    lanes = lax.broadcasted_iota(jnp.int32, (SUB, LANES), 1)
    edge_total[...] = jnp.zeros((SUB, LANES), jnp.float32)

    @pl.when(has_next)
    def _():
        at = rows - 1
        column = lax.broadcasted_iota(jnp.int32, (LANES, LANES), 0)
        chosen = jnp.logical_and(
            lax.rem(column, SUB) == SUB - 1, label_ref[pl.ds(at, 1), :] == column // SUB
        )
        member = chosen.astype(jnp.float32).astype(jnp.bfloat16)
        velocity = flow[:, at, :].reshape(planes // SUB, SUB, LANES)
        mean_velocity = both_halves(jnp.sum(velocity, axis=0)) * (1.0 / snapshots)
        here = warmth[:, at, :]
        halo_copy.wait_recv()
        limit = jnp.minimum(depth[pl.ds(at, 1), :], halo_in[pl.ds(planes, 1), :])
        wet = (lax.rem(sub, levels).astype(jnp.float32) < limit).astype(jnp.float32)
        point = (0.5 * (here + halo_in[pl.ds(0, planes), :])).reshape(planes // SUB, SUB, LANES)
        mean_warmth = both_halves(jnp.sum(point, axis=0)) * (1.0 / snapshots)
        cross = both_halves(
            jnp.sum((velocity - mean_velocity) * (point - mean_warmth), axis=0)
        ) * (1.0 / snapshots)
        average[:, at, :] = mean_warmth[:levels]
        depth[pl.ds(rows, SUB), :] = halo_in[pl.ds(planes, SUB), :]
        values = jnp.concatenate(
            [
                (point * wet).reshape(planes, LANES),
                wet,
                (velocity * wet).reshape(planes, LANES),
                jnp.where(sub < levels, mean_velocity * mean_warmth, cross) * wet,
            ],
            axis=0,
        )
        zonal = split_dot(values, member)
        edge_sums[...] = sums_of(zonal)
        each_peer(lambda to: edge_copy(to, me).start())
        parts = [zonal[SUB * n : SUB * (n + 1)] for n in range(fields // SUB)]
        first = parts[0]
        for n in range(1, SUB):
            first = first + pltpu.roll(parts[n], LANES - n, 1)
        second = parts[SUB]
        for n in range(SUB + 1, fields // SUB):
            second = second + pltpu.roll(parts[n], LANES - (n - SUB), 1)
        edge_stats[...] = jnp.concatenate([first, second], axis=0)

        @pl.when(me < lon_devices - 1)
        def _():
            edge_stat_copy(me).start()

    add_pair(1)
    send_group_stats(1)

    def block_eddy(b, block_sums):
        at = pl.ds(b * SUB, SUB)
        wet = wet_cells(b)
        index = label_ref[at, :] * SUB + sub
        bar = block_sums / jnp.maximum(pltpu.roll(block_sums, levels, 0), 1.0)
        for k in range(levels):
            cells = jnp.take_along_axis(
                jnp.broadcast_to(bar[k : k + 1], (SUB, LANES)), index, axis=1
            )
            eddy_ref[k, at, :] = wet[k] * (average[k, at, :] - cells)

    def add_sums(d, total):
        source = lax.rem(chip + chips - d, chips)
        return total + peer_sums[pl.ds(source, 1)][0]

    await_bytes(peer_sums.at[pl.ds(0, chips - 1)], sum_recv)
    all_sums[mine] = lax.fori_loop(1, chips, add_sums, chip_sums[...], unroll=chips <= SUB)
    if parities == 2:
        share_copy.start()

    def write_transport(total, early):
        half = packed // 2
        lane = lax.broadcasted_iota(jnp.int32, (half, LANES), 1)
        total = jnp.concatenate(
            [
                total,
                jnp.where(
                    lane < LANES - used,
                    pltpu.roll(total[:half], LANES - used, 1),
                    pltpu.roll(total[half:], 2 * LANES - 2 * used, 1),
                ),
            ],
            axis=0,
        )
        extra = None if early else edge_stats_total[...]
        edge_lane = lax.rem(lanes, SUB) == SUB - 1
        pieces = []
        for n in range(fields // SUB):
            piece = total[SUB * n : SUB * (n + 1)]
            if extra is not None:
                part = extra[:SUB] if n < SUB else extra[SUB:]
                if n % SUB:
                    part = pltpu.roll(part, n % SUB, 1)
                piece = piece + jnp.where(edge_lane, part, 0.0)
            pieces.append(piece)
        shape = (planes // SUB, SUB, LANES)
        per = planes // SUB
        count = pieces[per]
        divisor = jnp.maximum(count, 1.0)
        means_t = jnp.stack(pieces[:per]) / divisor
        means_v = jnp.stack(pieces[per + 1 : 2 * per + 1]) / divisor
        bar_v = both_halves(jnp.sum(means_v, axis=0)) * (1.0 / snapshots)
        bar_t = both_halves(jnp.sum(means_t, axis=0)) * (1.0 / snapshots)
        swing = both_halves(jnp.sum((means_v - bar_v) * (means_t - bar_t), axis=0)) * (1.0 / snapshots)
        upper = jnp.where(sub < levels, scaling * count * bar_v * bar_t, scaling * count * swing)
        lower = scaling * pieces[2 * per + 1] - upper
        if owners > 1:
            shift = LANES - lax.rem(me, owners) * share_rows
            upper = pltpu.roll(upper, shift, 1)
            lower = pltpu.roll(lower, shift, 1)
        spread = lax.rem(lanes * SUB + sub, LANES)
        for c, part in enumerate((upper, lower, upper, lower)):
            for k in range(levels):
                row = c // 2 * levels + k
                table = jnp.take_along_axis(
                    jnp.broadcast_to(part[row : row + 1], (SUB, LANES)), spread, axis=1
                )
                transport_ref[c, k] = table[:share_rows, :BASINS]

    def add_received(d, total):
        source = lax.rem(chip + chips - d, chips)
        return total + received[pl.ds(source, 1)][0]

    if parities == 2:
        share_copy.wait_recv()
    for b in range(last):
        block_eddy(b, all_sums[b % parities, b // parities])

    await_bytes(received.at[pl.ds(0, chips - 1)], stat_recv)
    total = lax.fori_loop(
        1, chips, add_received, chip_stats[pl.ds(own_slot, 1)][0], unroll=chips <= SUB
    )
    late = jnp.logical_and(has_next, me == lon_devices - 1)

    @pl.when(jnp.logical_not(late))
    def _():
        write_transport(total, True)

    @pl.when(has_next)
    def _():
        def add_edge(d, total):
            source = lax.rem(me + lon_devices - d, lon_devices)
            return total + peer_edge[pl.ds(source, 1)][0]

        await_bytes(peer_edge.at[pl.ds(0, lon_devices - 1)], edge_recv)
        edge_total[...] = lax.fori_loop(
            1, lon_devices, add_edge, edge_sums[...], unroll=lon_devices <= SUB
        )

    block_eddy(last, all_sums[last % parities, last // parities] + edge_total[...])
    @pl.when(late)
    def _():
        def add_edge_stats(d, total):
            source = lax.rem(me + lon_devices - d, lon_devices)
            return total + peer_edge_stats[pl.ds(source, 1)][0]

        await_bytes(peer_edge_stats.at[pl.ds(0, lon_devices - 1)], edge_stat_recv)
        edge_stats_total[...] = lax.fori_loop(
            1, lon_devices, add_edge_stats, edge_stats[...], unroll=lon_devices <= SUB
        )
        write_transport(total, False)

    @pl.when(lat > 0)
    def _():
        halo_copy.wait_send()

    sums_pair_copy.wait_send()
    await_bytes(pair_stats, pair_send)
    await_bytes(peer_sums.at[pl.ds(0, chips - 1)], sum_send)
    await_bytes(received.at[pl.ds(0, chips - 1)], stat_send)
    if parities == 2:
        share_copy.wait_send()

    @pl.when(has_next)
    def _():
        await_bytes(peer_edge.at[pl.ds(0, lon_devices - 1)], edge_send)

        @pl.when(me < lon_devices - 1)
        def _():
            edge_stat_copy(me).wait_send()


def store(eddy_ref, transport_ref, eddy_hbm, transport_hbm, sems):
    copies = (
        pltpu.make_async_copy(eddy_ref, eddy_hbm, sems.at[0]),
        pltpu.make_async_copy(transport_ref, transport_hbm, sems.at[1]),
    )
    for copy in copies:
        copy.start()
    for copy in copies:
        copy.wait()


def shards(
    lat_devices, lon_devices,
    poleward_flow, potential_warmth, water_profile_flag, floor_count, catchment_label_for_site,
):
    snapshots, levels, rows, columns = poleward_flow.shape
    share_rows = rows // lon_devices
    blocks = rows // SUB
    planes = snapshots * levels
    fields = 2 * planes + 4 * levels
    packed = fields * 2 // 3
    chips = lon_devices // 2
    parities = 2 if share_rows == SUB else 1
    slots = blocks // parities
    f32, i32, vmem, dma = jnp.float32, jnp.int32, pltpu.VMEM, pltpu.SemaphoreType.DMA
    eddy_shape = (levels, rows, columns)
    transport_shape = (4, levels, share_rows, BASINS)
    eddy_temp, transport = pl.pallas_call(
        functools.partial(kernel, lat_devices, lon_devices, snapshots, levels, share_rows),
        out_shape=(vmem(eddy_shape, f32), vmem(transport_shape, f32)),
        in_specs=[pl.BlockSpec(memory_space=pltpu.HBM)] * 5,
        out_specs=(pl.BlockSpec(memory_space=vmem), pl.BlockSpec(memory_space=vmem)),
        scratch_shapes=[
            vmem((3, rows, columns), i32),
            vmem((rows + SUB, columns), f32),
            vmem((planes, rows, columns), f32),
            vmem((planes, rows + SUB, columns), f32),
            vmem((levels, rows, columns), f32),
            vmem((blocks, fields * SUB, LANES), f32),
            vmem((blocks, 2 * levels * SUB, LANES), f32),
            vmem((blocks, LANES, LANES), jnp.bfloat16),
            vmem((planes + SUB, LANES), f32),
            vmem((planes + SUB, LANES), f32),
            vmem((parities, slots, packed, LANES), f32),
            vmem((slots, packed, LANES), f32),
            vmem((slots, packed, LANES), f32),
            vmem((chips, packed, LANES), f32),
            vmem((parities, slots, SUB, LANES), f32),
            vmem((slots, SUB, LANES), f32),
            vmem((slots, SUB, LANES), f32),
            vmem((chips, slots, SUB, LANES), f32),
            vmem((parities, slots, SUB, LANES), f32),
            vmem((SUB, LANES), f32),
            vmem((lon_devices, SUB, LANES), f32),
            vmem((2 * SUB, LANES), f32),
            vmem((lon_devices, 2 * SUB, LANES), f32),
            vmem((SUB, LANES), f32),
            vmem((2 * SUB, LANES), f32),
            dma,
            dma,
            dma((GROUPS,)),
            dma,
            dma,
            dma,
            dma,
            dma,
            dma((GROUPS,)),
            dma,
            dma,
            dma,
            dma,
            dma,
            dma,
            dma,
            dma,
            dma,
            dma,
        ],
        compiler_params=pltpu.CompilerParams(
            collective_id=0, has_side_effects=True, vmem_limit_bytes=62 * 1024 * 1024
        ),
        name="heat_transport",
    )(
        poleward_flow.reshape(planes, rows, columns),
        potential_warmth.reshape(planes, rows, columns),
        water_profile_flag,
        floor_count,
        catchment_label_for_site,
    )
    eddy_temp, transport = pl.pallas_call(
        store,
        out_shape=(
            jax.ShapeDtypeStruct(eddy_shape, f32), jax.ShapeDtypeStruct(transport_shape, f32)
        ),
        in_specs=[pl.BlockSpec(memory_space=vmem)] * 2,
        out_specs=(pl.BlockSpec(memory_space=pltpu.HBM), pl.BlockSpec(memory_space=pltpu.HBM)),
        scratch_shapes=[dma((2,))],
        name="store_results",
    )(
        pltpu.with_memory_space_constraint(eddy_temp, vmem),
        pltpu.with_memory_space_constraint(transport, vmem),
    )
    return eddy_temp, jnp.transpose(transport, (0, 3, 1, 2))


def solution(mesh):
    return jax.shard_map(
        functools.partial(shards, mesh.shape["lat"], mesh.shape["lon"]),
        mesh=mesh,
        in_specs=(
            P(None, None, "lat", "lon"),
            P(None, None, "lat", "lon"),
            P("lat", "lon"),
            P("lat", "lon"),
            P("lat", "lon"),
        ),
        out_specs=(P(None, "lat", "lon"), P(None, None, None, ("lat", "lon"))),
        check_vma=False,
    )
```

```python
import functools
import math

import jax
import jax.numpy as jnp
from jax import lax
from jax.experimental import pallas as pl
from jax.experimental.pallas import tpu as pltpu
from jax.sharding import PartitionSpec as P

BASINS = 10
MESH = pl.DeviceIdType.MESH
SUB = 8
LANES = 128
GROUPS = 2


def kernel(
    lat_devices, lon_devices, snapshots, levels, share_rows,
    flow_hbm, warmth_hbm, flag_hbm, floor_hbm, label_hbm,
    eddy_ref, transport_ref,
    columns, depth, flow, warmth, average, members,
    halo_out, halo_in, stats, pair_stats, chip_stats, received, sums, pair_sums, chip_sums, peer_sums, all_sums,
    edge_sums, peer_edge, edge_stats, peer_edge_stats, edge_total, edge_stats_total,
    load_first, load_warmth, load_flow, halo_send, halo_recv,
    sums_pair_send, sums_pair_recv, pair_send, pair_recv, stat_send, stat_recv, sum_send, sum_recv, share_send, share_recv,
    edge_send, edge_recv, edge_stat_send, edge_stat_recv,
):
    rows = flow.shape[0]
    blocks = rows // SUB
    last = blocks - 1
    half_blocks = blocks // GROUPS
    label_ref = columns.at[2]
    owners = SUB // share_rows
    planes = snapshots * levels
    parities, slots, packed = stats.shape[:3]
    group_slots = slots // GROUPS
    fields = packed * 3 // 2
    used = BASINS * SUB
    chips = lon_devices // 2
    lat = lax.axis_index("lat")
    me = lax.axis_index("lon")
    core = lax.rem(me, 2)
    chip = me // 2
    mine = core if parities == 2 else 0
    theirs = 1 - core if parities == 2 else 0
    partner = (lat, me + 1 - 2 * core)
    own_slot = me // (owners * parities)
    scaling = 1.0 / math.sqrt(LANES * lon_devices)
    has_next = lat < lat_devices - 1

    def window(b):
        return pl.ds(b * SUB, SUB)

    group_rows = half_blocks * SUB

    def load_rows(source, target, first, count, sem):
        at = pl.ds(first, count)
        for n in range(planes):
            pltpu.make_async_copy(source.at[n, at, :], target.at[at, n, :], sem).start()

    def await_bytes(ref, sem):
        pltpu.make_async_copy(ref, ref, sem).wait()

    for n, column in enumerate((flag_hbm, floor_hbm, label_hbm)):
        pltpu.make_async_copy(column, columns.at[n], load_first).start()
    pltpu.make_async_copy(warmth_hbm.at[:, 0, :], warmth.at[0], load_first).start()
    for n in range(1, SUB):
        pltpu.make_async_copy(warmth_hbm.at[:, n, :], warmth.at[n], load_warmth).start()
    load_rows(warmth_hbm, warmth, SUB, rows - SUB, load_warmth)

    barrier = pltpu.get_barrier_semaphore()

    def greet(d, carry):
        pl.semaphore_signal(
            barrier, inc=1, device_id=(lat, lax.rem(me + d, lon_devices)), device_id_type=MESH
        )
        return carry

    @pl.when(has_next)
    def _():
        pl.semaphore_signal(barrier, inc=1, device_id=(lat + 1, me), device_id_type=MESH)

    lax.fori_loop(1, lon_devices, greet, 0)
    for g in range(GROUPS):
        load_rows(flow_hbm, flow, g * group_rows, group_rows, load_flow.at[g])

    halo_copy = pltpu.make_async_remote_copy(
        src_ref=halo_out, dst_ref=halo_in, send_sem=halo_send, recv_sem=halo_recv,
        device_id=(jnp.maximum(lat - 1, 0), me), device_id_type=MESH,
    )

    def group(g):
        return pl.ds(g * group_slots, group_slots)

    def pair_copy(g):
        return pltpu.make_async_remote_copy(
            src_ref=stats.at[theirs, group(g)], dst_ref=pair_stats.at[group(g)],
            send_sem=pair_send, recv_sem=pair_recv.at[g],
            device_id=partner, device_id_type=MESH,
        )

    sums_pair_copy = pltpu.make_async_remote_copy(
        src_ref=sums.at[theirs], dst_ref=pair_sums,
        send_sem=sums_pair_send, recv_sem=sums_pair_recv, device_id=partner, device_id_type=MESH,
    )

    def sum_copy(to, source):
        return pltpu.make_async_remote_copy(
            src_ref=chip_sums, dst_ref=peer_sums.at[source],
            send_sem=sum_send, recv_sem=sum_recv,
            device_id=(lat, 2 * to + core), device_id_type=MESH,
        )

    def stat_slot(to):
        return (2 * to + core) // (owners * parities)

    def stat_copy(to, source):
        return pltpu.make_async_remote_copy(
            src_ref=chip_stats.at[stat_slot(to)], dst_ref=received.at[source],
            send_sem=stat_send, recv_sem=stat_recv,
            device_id=(lat, 2 * to + core), device_id_type=MESH,
        )

    share_copy = pltpu.make_async_remote_copy(
        src_ref=all_sums.at[mine], dst_ref=all_sums.at[mine],
        send_sem=share_send, recv_sem=share_recv, device_id=partner, device_id_type=MESH,
    )

    def edge_copy(to, source):
        return pltpu.make_async_remote_copy(
            src_ref=edge_sums, dst_ref=peer_edge.at[source],
            send_sem=edge_send, recv_sem=edge_recv,
            device_id=(lat, to), device_id_type=MESH,
        )

    def edge_stat_copy(source):
        return pltpu.make_async_remote_copy(
            src_ref=edge_stats, dst_ref=peer_edge_stats.at[source],
            send_sem=edge_stat_send, recv_sem=edge_stat_recv,
            device_id=(lat, lon_devices - 1), device_id_type=MESH,
        )

    def each_chip(action):
        def step(d, carry):
            action(lax.rem(chip + d, chips))
            return carry

        lax.fori_loop(1, chips, step, 0)

    def each_peer(action):
        def step(d, carry):
            action(lax.rem(me + d, lon_devices))
            return carry

        lax.fori_loop(1, lon_devices, step, 0)

    sub = lax.broadcasted_iota(jnp.int32, (SUB, LANES), 0)
    level = lax.broadcasted_iota(jnp.int32, (levels, SUB, LANES), 0).astype(jnp.float32)

    def next_row(here, after):
        first = lax.broadcasted_iota(jnp.int32, here.shape, here.ndim - 2) == 0
        return pltpu.roll(jnp.where(first, after, here), SUB - 1, here.ndim - 2)

    def both_halves(x):
        return x + pltpu.roll(x, levels, 0)

    level_of = lax.rem(sub, levels).astype(jnp.float32)

    def wet_cells(b):
        here = depth[window(b), :]
        limit = jnp.minimum(here, next_row(here, depth[window(b + 1), :]))
        return (level < limit[None]).astype(jnp.float32)

    def split_dot(values, member):
        high = values.astype(jnp.bfloat16)
        low = (values - high.astype(jnp.float32)).astype(jnp.bfloat16)
        return lax.dot_general(
            jnp.concatenate([high, low], axis=1), jnp.concatenate([member, member], axis=1),
            (((1,), (1,)), ((), ())), preferred_element_type=jnp.float32,
        )

    def by_row(products, count):
        products = products.reshape(SUB, count, LANES)
        row_of = lax.rem(lax.broadcasted_iota(jnp.int32, (count, LANES), 1), SUB)
        zonal = products[0]
        for j in range(1, SUB):
            zonal = jnp.where(row_of == j, products[j], zonal)
        return zonal

    def wet_row(j):
        limit = jnp.minimum(depth[pl.ds(j, 1), :], depth[pl.ds(j + 1, 1), :])
        return (level_of < limit).astype(jnp.float32)

    def tiles(x):
        return x.reshape(planes // SUB, SUB, LANES)

    def block_means(b):
        labels = label_ref[window(b), :]
        member = jnp.concatenate(
            [(labels == n).astype(jnp.float32) for n in range(LANES // SUB)], axis=0
        ).astype(jnp.bfloat16)
        members[b] = member
        sums_of_row = [
            both_halves(jnp.sum(tiles(warmth[j]), axis=0)) for j in range(b * SUB, (b + 1) * SUB + 1)
        ]
        values = []
        for n in range(SUB):
            j = b * SUB + n
            mean_warmth = (sums_of_row[n] + sums_of_row[n + 1]) * (0.5 / snapshots)
            average[pl.ds(j * SUB, SUB), :] = mean_warmth
            values.append(jnp.where(sub < levels, mean_warmth, 1.0) * wet_row(j))
        products = split_dot(jnp.concatenate(values, axis=0), member)
        sums[b % parities, b // parities] = by_row(products, SUB)

    def row_values(velocity, point, mean_warmth, wet):
        mean_velocity = both_halves(jnp.sum(velocity, axis=0)) * (1.0 / snapshots)
        cross = both_halves(
            jnp.sum((velocity - mean_velocity) * (point - 2.0 * mean_warmth), axis=0)
        ) * (0.5 / snapshots)
        return jnp.concatenate(
            [
                (point * (0.5 * wet)).reshape(planes, LANES),
                wet,
                (velocity * wet).reshape(planes, LANES),
                jnp.where(sub < levels, mean_velocity * mean_warmth, cross) * wet,
            ],
            axis=0,
        )

    def block_stats(b):
        values = []
        for j in range(b * SUB, (b + 1) * SUB):
            values.append(
                row_values(
                    tiles(flow[j]), tiles(warmth[j] + warmth[j + 1]),
                    average[pl.ds(j * SUB, SUB), :], wet_row(j),
                )
            )
        zonal = by_row(split_dot(jnp.concatenate(values, axis=0), members[b]), fields)
        half = packed // 2
        rest = zonal[packed:]
        spare = lax.broadcasted_iota(jnp.int32, (half, LANES), 1) >= used
        stats[b % parities, b // parities] = jnp.concatenate(
            [
                jnp.where(spare, pltpu.roll(rest, used, 1), zonal[:half]),
                jnp.where(spare, pltpu.roll(rest, 2 * used - LANES, 1), zonal[half:packed]),
            ],
            axis=0,
        )

    def sums_of(zonal):
        warmth_sum = both_halves(jnp.sum(zonal[:planes].reshape(planes // SUB, SUB, LANES), axis=0))
        return jnp.where(sub < levels, warmth_sum * (1.0 / snapshots), zonal[planes : planes + SUB])

    def add_pair(g):
        pair_copy(g).wait_recv()
        for s in range(g * group_slots, (g + 1) * group_slots):
            chip_stats[s] = stats[mine, s] + pair_stats[s]

    def send_sums():
        sums_pair_copy.wait_recv()
        chip_sums[...] = sums[mine] + pair_sums[...]
        each_chip(lambda to: sum_copy(to, chip).start())

    def send_group_stats(g):
        def send_stats(to):
            @pl.when(stat_slot(to) // group_slots == g)
            def _():
                stat_copy(to, chip).start()

        each_chip(send_stats)

    await_bytes(columns, load_first)
    await_bytes(warmth.at[0], load_first)
    depth[pl.ds(0, rows), :] = (columns[0] * columns[1]).astype(jnp.float32)
    depth[pl.ds(rows, SUB), :] = jnp.zeros((SUB, LANES), jnp.float32)
    warmth[rows] = jnp.zeros((planes, LANES), jnp.float32)
    halo_out[pl.ds(0, planes), :] = warmth[0]
    halo_out[pl.ds(planes, SUB), :] = depth[pl.ds(0, SUB), :]

    pl.semaphore_wait(barrier, lon_devices - 1 + (lat > 0).astype(jnp.int32))

    @pl.when(lat > 0)
    def _():
        halo_copy.start()

    await_bytes(warmth.at[pl.ds(0, rows - 1)], load_warmth)
    for b in range(blocks):
        block_means(b)
    sums_pair_copy.start()
    await_bytes(flow.at[pl.ds(0, group_rows)], load_flow.at[0])
    for b in range(half_blocks):
        block_stats(b)
    pair_copy(0).start()
    @pl.when(core == 0)
    def _():
        send_sums()

    await_bytes(flow.at[pl.ds(0, group_rows)], load_flow.at[1])
    for b in range(half_blocks, blocks):
        block_stats(b)
    pair_copy(1).start()

    @pl.when(core == 1)
    def _():
        send_sums()

    add_pair(0)
    send_group_stats(0)

    lanes = lax.broadcasted_iota(jnp.int32, (SUB, LANES), 1)
    edge_total[...] = jnp.zeros((SUB, LANES), jnp.float32)

    @pl.when(has_next)
    def _():
        at = rows - 1
        column = lax.broadcasted_iota(jnp.int32, (LANES, LANES), 0)
        chosen = jnp.logical_and(
            lax.rem(column, SUB) == SUB - 1, label_ref[pl.ds(at, 1), :] == column // SUB
        )
        member = chosen.astype(jnp.float32).astype(jnp.bfloat16)
        halo_copy.wait_recv()
        depth[pl.ds(rows, SUB), :] = halo_in[pl.ds(planes, SUB), :]
        point = tiles(warmth[at] + halo_in[pl.ds(0, planes), :])
        mean_warmth = both_halves(jnp.sum(point, axis=0)) * (0.5 / snapshots)
        average[pl.ds(at * SUB, SUB), :] = mean_warmth
        values = row_values(tiles(flow[at]), point, mean_warmth, wet_row(at))
        zonal = split_dot(values, member)
        edge_sums[...] = sums_of(zonal)
        each_peer(lambda to: edge_copy(to, me).start())
        parts = [zonal[SUB * n : SUB * (n + 1)] for n in range(fields // SUB)]
        first = parts[0]
        for n in range(1, SUB):
            first = first + pltpu.roll(parts[n], LANES - n, 1)
        second = parts[SUB]
        for n in range(SUB + 1, fields // SUB):
            second = second + pltpu.roll(parts[n], LANES - (n - SUB), 1)
        edge_stats[...] = jnp.concatenate([first, second], axis=0)

        @pl.when(me < lon_devices - 1)
        def _():
            edge_stat_copy(me).start()

    add_pair(1)
    send_group_stats(1)

    def block_eddy(b, block_sums):
        at = pl.ds(b * SUB, SUB)
        wet = wet_cells(b)
        index = label_ref[at, :] * SUB + sub
        bar = block_sums / jnp.maximum(pltpu.roll(block_sums, levels, 0), 1.0)
        for k in range(levels):
            cells = jnp.take_along_axis(
                jnp.broadcast_to(bar[k : k + 1], (SUB, LANES)), index, axis=1
            )
            mean_warmth = average[pl.ds(b * SUB * SUB + k, SUB, stride=SUB), :]
            eddy_ref[k, at, :] = wet[k] * (mean_warmth - cells)

    def add_sums(d, total):
        source = lax.rem(chip + chips - d, chips)
        return total + peer_sums[pl.ds(source, 1)][0]

    await_bytes(peer_sums.at[pl.ds(0, chips - 1)], sum_recv)
    all_sums[mine] = lax.fori_loop(1, chips, add_sums, chip_sums[...], unroll=chips <= SUB)
    if parities == 2:
        share_copy.start()

    def write_transport(total, early):
        half = packed // 2
        lane = lax.broadcasted_iota(jnp.int32, (half, LANES), 1)
        total = jnp.concatenate(
            [
                total,
                jnp.where(
                    lane < LANES - used,
                    pltpu.roll(total[:half], LANES - used, 1),
                    pltpu.roll(total[half:], 2 * LANES - 2 * used, 1),
                ),
            ],
            axis=0,
        )
        extra = None if early else edge_stats_total[...]
        edge_lane = lax.rem(lanes, SUB) == SUB - 1
        pieces = []
        for n in range(fields // SUB):
            piece = total[SUB * n : SUB * (n + 1)]
            if extra is not None:
                part = extra[:SUB] if n < SUB else extra[SUB:]
                if n % SUB:
                    part = pltpu.roll(part, n % SUB, 1)
                piece = piece + jnp.where(edge_lane, part, 0.0)
            pieces.append(piece)
        shape = (planes // SUB, SUB, LANES)
        per = planes // SUB
        count = pieces[per]
        divisor = jnp.maximum(count, 1.0)
        means_t = jnp.stack(pieces[:per]) / divisor
        means_v = jnp.stack(pieces[per + 1 : 2 * per + 1]) / divisor
        bar_v = both_halves(jnp.sum(means_v, axis=0)) * (1.0 / snapshots)
        bar_t = both_halves(jnp.sum(means_t, axis=0)) * (1.0 / snapshots)
        swing = both_halves(jnp.sum((means_v - bar_v) * (means_t - bar_t), axis=0)) * (1.0 / snapshots)
        upper = jnp.where(sub < levels, scaling * count * bar_v * bar_t, scaling * count * swing)
        lower = scaling * pieces[2 * per + 1] - upper
        if owners > 1:
            shift = LANES - lax.rem(me, owners) * share_rows
            upper = pltpu.roll(upper, shift, 1)
            lower = pltpu.roll(lower, shift, 1)
        spread = lax.rem(lanes * SUB + sub, LANES)
        for c, part in enumerate((upper, lower, upper, lower)):
            for k in range(levels):
                row = c // 2 * levels + k
                table = jnp.take_along_axis(
                    jnp.broadcast_to(part[row : row + 1], (SUB, LANES)), spread, axis=1
                )
                transport_ref[c, k] = table[:share_rows, :BASINS]

    def add_received(d, total):
        source = lax.rem(chip + chips - d, chips)
        return total + received[pl.ds(source, 1)][0]

    if parities == 2:
        share_copy.wait_recv()
    for b in range(last):
        block_eddy(b, all_sums[b % parities, b // parities])

    await_bytes(received.at[pl.ds(0, chips - 1)], stat_recv)
    total = lax.fori_loop(
        1, chips, add_received, chip_stats[pl.ds(own_slot, 1)][0], unroll=chips <= SUB
    )
    late = jnp.logical_and(has_next, me == lon_devices - 1)

    @pl.when(jnp.logical_not(late))
    def _():
        write_transport(total, True)

    @pl.when(has_next)
    def _():
        def add_edge(d, total):
            source = lax.rem(me + lon_devices - d, lon_devices)
            return total + peer_edge[pl.ds(source, 1)][0]

        await_bytes(peer_edge.at[pl.ds(0, lon_devices - 1)], edge_recv)
        edge_total[...] = lax.fori_loop(
            1, lon_devices, add_edge, edge_sums[...], unroll=lon_devices <= SUB
        )

    block_eddy(last, all_sums[last % parities, last // parities] + edge_total[...])
    @pl.when(late)
    def _():
        def add_edge_stats(d, total):
            source = lax.rem(me + lon_devices - d, lon_devices)
            return total + peer_edge_stats[pl.ds(source, 1)][0]

        await_bytes(peer_edge_stats.at[pl.ds(0, lon_devices - 1)], edge_stat_recv)
        edge_stats_total[...] = lax.fori_loop(
            1, lon_devices, add_edge_stats, edge_stats[...], unroll=lon_devices <= SUB
        )
        write_transport(total, False)

    @pl.when(lat > 0)
    def _():
        halo_copy.wait_send()

    sums_pair_copy.wait_send()
    await_bytes(pair_stats, pair_send)
    await_bytes(peer_sums.at[pl.ds(0, chips - 1)], sum_send)
    await_bytes(received.at[pl.ds(0, chips - 1)], stat_send)
    if parities == 2:
        share_copy.wait_send()

    @pl.when(has_next)
    def _():
        await_bytes(peer_edge.at[pl.ds(0, lon_devices - 1)], edge_send)

        @pl.when(me < lon_devices - 1)
        def _():
            edge_stat_copy(me).wait_send()


def store(eddy_ref, transport_ref, eddy_hbm, transport_hbm, sems):
    copies = (
        pltpu.make_async_copy(eddy_ref, eddy_hbm, sems.at[0]),
        pltpu.make_async_copy(transport_ref, transport_hbm, sems.at[1]),
    )
    for copy in copies:
        copy.start()
    for copy in copies:
        copy.wait()


def shards(
    lat_devices, lon_devices,
    poleward_flow, potential_warmth, water_profile_flag, floor_count, catchment_label_for_site,
):
    snapshots, levels, rows, columns = poleward_flow.shape
    share_rows = rows // lon_devices
    blocks = rows // SUB
    planes = snapshots * levels
    fields = 2 * planes + 4 * levels
    packed = fields * 2 // 3
    chips = lon_devices // 2
    parities = 2 if share_rows == SUB else 1
    slots = blocks // parities
    f32, i32, vmem, dma = jnp.float32, jnp.int32, pltpu.VMEM, pltpu.SemaphoreType.DMA
    eddy_shape = (levels, rows, columns)
    transport_shape = (4, levels, share_rows, BASINS)
    eddy_temp, transport = pl.pallas_call(
        functools.partial(kernel, lat_devices, lon_devices, snapshots, levels, share_rows),
        out_shape=(vmem(eddy_shape, f32), vmem(transport_shape, f32)),
        in_specs=[pl.BlockSpec(memory_space=pltpu.HBM)] * 5,
        out_specs=(pl.BlockSpec(memory_space=vmem), pl.BlockSpec(memory_space=vmem)),
        scratch_shapes=[
            vmem((3, rows, columns), i32),
            vmem((rows + SUB, columns), f32),
            vmem((rows, planes, columns), f32),
            vmem((rows + 1, planes, columns), f32),
            vmem((rows * SUB, columns), f32),
            vmem((blocks, LANES, LANES), jnp.bfloat16),
            vmem((planes + SUB, LANES), f32),
            vmem((planes + SUB, LANES), f32),
            vmem((parities, slots, packed, LANES), f32),
            vmem((slots, packed, LANES), f32),
            vmem((slots, packed, LANES), f32),
            vmem((chips, packed, LANES), f32),
            vmem((parities, slots, SUB, LANES), f32),
            vmem((slots, SUB, LANES), f32),
            vmem((slots, SUB, LANES), f32),
            vmem((chips, slots, SUB, LANES), f32),
            vmem((parities, slots, SUB, LANES), f32),
            vmem((SUB, LANES), f32),
            vmem((lon_devices, SUB, LANES), f32),
            vmem((2 * SUB, LANES), f32),
            vmem((lon_devices, 2 * SUB, LANES), f32),
            vmem((SUB, LANES), f32),
            vmem((2 * SUB, LANES), f32),
            dma,
            dma,
            dma((GROUPS,)),
            dma,
            dma,
            dma,
            dma,
            dma,
            dma((GROUPS,)),
            dma,
            dma,
            dma,
            dma,
            dma,
            dma,
            dma,
            dma,
            dma,
            dma,
        ],
        compiler_params=pltpu.CompilerParams(
            collective_id=0, has_side_effects=True, vmem_limit_bytes=62 * 1024 * 1024
        ),
        name="heat_transport",
    )(
        poleward_flow.reshape(planes, rows, columns),
        potential_warmth.reshape(planes, rows, columns),
        water_profile_flag,
        floor_count,
        catchment_label_for_site,
    )
    eddy_temp, transport = pl.pallas_call(
        store,
        out_shape=(
            jax.ShapeDtypeStruct(eddy_shape, f32), jax.ShapeDtypeStruct(transport_shape, f32)
        ),
        in_specs=[pl.BlockSpec(memory_space=vmem)] * 2,
        out_specs=(pl.BlockSpec(memory_space=pltpu.HBM), pl.BlockSpec(memory_space=pltpu.HBM)),
        scratch_shapes=[dma((2,))],
        name="store_results",
    )(
        pltpu.with_memory_space_constraint(eddy_temp, vmem),
        pltpu.with_memory_space_constraint(transport, vmem),
    )
    return eddy_temp, jnp.transpose(transport, (0, 3, 1, 2))


def solution(mesh):
    return jax.shard_map(
        functools.partial(shards, mesh.shape["lat"], mesh.shape["lon"]),
        mesh=mesh,
        in_specs=(
            P(None, None, "lat", "lon"),
            P(None, None, "lat", "lon"),
            P("lat", "lon"),
            P("lat", "lon"),
            P("lat", "lon"),
        ),
        out_specs=(P(None, "lat", "lon"), P(None, None, None, ("lat", "lon"))),
        check_vma=False,
    )
```
